32 devices in a mesh: row: 4 (over y, core), col: 8 (over z, x).
Axes of the slice: x: 2, y: 2, z: 4, core: 2. Of those that a mesh axis runs over, the one named last changes fastest.
Arguments:
- tokens: bfloat16 [256, 2, 4096], P(None, None, 'row'), may hold values from -6 to 6
- task_emb: bfloat16 [512, 1024], replicated, may hold values from -6 to 6
- gen_in: bfloat16 [1024, 512], replicated, may hold values from -0.1875 to 0.1875
- gen_a: bfloat16 [512, 4096, 16], P(None, ('row', 'col')), may hold values from -0.0078125 to 0.0078125
- gen_b: bfloat16 [512, 16, 14336], P(None, 'row', 'col'), may hold values from -0.125 to 0.125
- w_gate: bfloat16 [4096, 14336], P('row', 'col'), may hold values from -0.09375 to 0.09375
- w_up: bfloat16 [4096, 14336], P('row', 'col'), may hold values from -0.09375 to 0.09375
- w_down: bfloat16 [14336, 4096], P('col', 'row'), may hold values from -0.046875 to 0.046875
- group_count: int32 [64], replicated, may hold values from 1 to 16, 256 in all
- group_task: int32 [64], replicated, may hold values from 0 to 511, as said below
Outputs:
- mixed: bfloat16 [256, 2, 4096], P('col', None, 'row')
The draws below stay inside these ranges and needn't reach their ends.
Inputs may be any that keep to these rules, and one draw needn't show every extreme that they name: `group_count`: requests in each group, in the order of the requests; they sum to 256 and the largest is 16. `group_task`: distinct task ids, one for each group.
All inputs are finite; a program needn't handle non-finite values.
Results may differ from the reference program's by a relative error of at most 0.0078.
Values may be sent and summed in bfloat16 or wider, within the bound.
No kernel may reach another device: no remote copies, remote signals or barrier semaphores. Data moves between devices by JAX's collectives and lax.ppermute only.
A program may use at most 128 MiB of HBM per device.

```python
import math
import jax
import jax.numpy as jnp
import numpy as np

D = 4096
HIDDEN_UNITS = 14336
RANK = 16
EMB = 1024
HYPER = 512
TASKS = 512
GROUPS = 64
MOST = 16
REQUEST_COUNT = 256
DRAFT_TOKENS = 2


def draw_group_task(key, part):
    return jax.random.permutation(key, TASKS)[:GROUPS].astype(jnp.int32)


def block_levels(stream_key, shape, cuts, least, high):
    def one(dim, blocks):
        draws = jax.random.uniform(jax.random.fold_in(jax.random.fold_in(stream_key, 6), dim), (blocks,), jnp.float32, least / len(cuts), high / len(cuts))
        return jnp.repeat(jnp.exp(draws), shape[dim] // blocks).reshape((-1,) + (1,) * (len(shape) - dim - 1))

    level = one(*cuts[0])
    for cut in cuts[1:]:
        level = level * one(*cut)
    return level


def length_profile(number_of, total, limit, skew):
    weights = [(1 << 20) // math.isqrt(rank ** skew) + 1 for rank in range(2, number_of + 1)]
    rest, given = total - limit - (number_of - 1), [1] * (number_of - 1)
    while rest > 0:
        movable = [i for i in range(number_of - 1) if given[i] < limit]
        whole, budget = sum([weights[i] for i in movable]), rest
        for i in movable:
            addition = min(limit - given[i], max(1, budget * weights[i] // whole), rest)
            given[i] = given[i] + addition
            rest = rest - addition
    return np.array([limit] + given)


def uneven(own_key, number_of, total, limit, skew):
    if number_of == 2:
        one = jax.random.randint(own_key, (), max(1, total - limit), min(limit, total - 1) + 1)
        return jnp.stack([one, total - one])
    tallies = jnp.asarray(length_profile(number_of, total, limit, skew), jnp.int32)
    couples = (number_of - 1) // 2
    giver, sink = tallies[1:1 + 2 * couples:2], tallies[2:2 + 2 * couples:2]
    room = jnp.minimum(giver - 1, limit - sink)
    passed = jax.random.randint(jax.random.fold_in(own_key, 1), (couples,), 0, 1 << 20) % (room + 1)
    tallies = tallies.at[1:1 + 2 * couples:2].set(giver - passed).at[2:2 + 2 * couples:2].set(sink + passed)
    return tallies[jax.random.permutation(jax.random.fold_in(own_key, 2), number_of)]


def scatter_about(key, extent, width, reach, shards=(), kind=jnp.bfloat16):
    entries = jax.random.normal(key, extent, jnp.float32) * width
    if len(shards) > 0:
        entries = block_levels(key, extent, shards, -0.22, 0.18) * entries
    return jnp.clip(entries, min=-reach, max=reach).astype(kind)


def setup_inputs(seed: int = 0) -> dict:
    arg_keys = jax.random.split(jax.random.key(seed), 11)
    tokens = scatter_about(arg_keys[0], (REQUEST_COUNT, DRAFT_TOKENS, D), 1.0, 6.0, ((2, 4),))
    task_emb = scatter_about(arg_keys[1], (TASKS, EMB), 1.0, 6.0)
    gen_in = scatter_about(arg_keys[2], (EMB, HYPER), EMB ** -0.5, 0.1875)
    gen_a = scatter_about(arg_keys[3], (HYPER, D, RANK), (HYPER * D // 4) ** -0.5, 0.0078125, ((1, 32),))
    gen_b = scatter_about(arg_keys[4], (HYPER, RANK, HIDDEN_UNITS), (HYPER * RANK // 4) ** -0.5, 0.125, ((1, 4), (2, 8)))
    w_gate = scatter_about(arg_keys[5], (D, HIDDEN_UNITS), D ** -0.5, 0.09375, ((0, 4), (1, 8)))
    w_up = scatter_about(arg_keys[6], (D, HIDDEN_UNITS), D ** -0.5, 0.09375, ((0, 4), (1, 8)))
    w_down = scatter_about(arg_keys[7], (HIDDEN_UNITS, D), HIDDEN_UNITS ** -0.5, 0.046875, ((0, 8), (1, 4)))
    group_count = uneven(arg_keys[8], GROUPS, REQUEST_COUNT, MOST, 2).astype(jnp.int32)
    group_task = draw_group_task(jax.random.fold_in(arg_keys[10], 71), 0)
    return {"tokens": tokens, "task_emb": task_emb, "gen_in": gen_in, "gen_a": gen_a, "gen_b": gen_b, "w_gate": w_gate, "w_up": w_up, "w_down": w_down, "group_count": group_count, "group_task": group_task}


def reference(tokens, task_emb, gen_in, gen_a, gen_b, w_gate, w_up, w_down, group_count, group_task):
    group_ends = jnp.cumsum(group_count).astype(jnp.int32)
    request_ids = jnp.arange(REQUEST_COUNT, dtype=jnp.int32)
    request_group = jnp.sum((request_ids[:, None] >= group_ends[None, :]).astype(jnp.int32), axis=1).astype(jnp.int32)
    chosen = task_emb[group_task]
    hyper_out = jax.nn.silu(jnp.dot(chosen, gen_in, preferred_element_type=jnp.float32)).astype(jnp.bfloat16)
    factor_a = jnp.dot(hyper_out, gen_a.reshape(HYPER, D * RANK), preferred_element_type=jnp.float32).astype(jnp.bfloat16).reshape(GROUPS, D, RANK)
    second_factor = jnp.dot(hyper_out, gen_b.reshape(HYPER, RANK * HIDDEN_UNITS), preferred_element_type=jnp.float32).astype(jnp.bfloat16).reshape(GROUPS, RANK, HIDDEN_UNITS)
    flat_tokens = tokens.reshape(REQUEST_COUNT * DRAFT_TOKENS, D)
    gate_total = jnp.dot(flat_tokens, w_gate, preferred_element_type=jnp.float32)
    up_total = jnp.dot(flat_tokens, w_up, preferred_element_type=jnp.float32)
    reduced_rank_term = jnp.einsum("bsd,bdr->bsr", tokens.astype(jnp.float32), factor_a[request_group].astype(jnp.float32)).astype(jnp.bfloat16)
    adapter_update = jnp.einsum("klv,kve->kle", reduced_rank_term.astype(jnp.float32), second_factor[request_group].astype(jnp.float32))
    adapter_update = adapter_update.reshape(REQUEST_COUNT * DRAFT_TOKENS, HIDDEN_UNITS)
    hidden_state = (jax.nn.silu(gate_total) * (up_total + adapter_update)).astype(jnp.bfloat16)
    mixed = jnp.dot(hidden_state, w_down, preferred_element_type=jnp.float32).astype(jnp.bfloat16)
    return mixed.reshape(REQUEST_COUNT, DRAFT_TOKENS, D)
```

```python
import jax
import jax.numpy as jnp
from jax import lax
from jax.sharding import PartitionSpec as P

F32 = jnp.float32
BF16 = jnp.bfloat16


def swap(x, axis, mask):
    n = lax.axis_size(axis)
    return lax.ppermute(x, axis, [(i, i ^ mask) for i in range(n)])


def masks_of(n):
    return [1 << b for b in range(n.bit_length() - 1)]


def col_masks(n):
    out, seen = [], 0
    for b in range(n.bit_length() - 1):
        if b == 0:
            out.append(1)
        else:
            seen |= 1 << b
            out.append(seen if b <= 2 else 1 << b)
    return out


def dest_order(n, masks):
    order = []
    for p in range(n):
        d = 0
        for s, m in enumerate(masks):
            if (p >> s) & 1:
                d ^= m
        order.append(d)
    return order


def pick(x, i, axis=0):
    return lax.dynamic_index_in_dim(x, i, axis, keepdims=False)


CHUNKS = 2


def shards(tokens, task_emb, gen_in, gen_a, gen_b, w_gate, w_up, w_down, group_count, group_task):
    batch, draft, width = tokens.shape
    rows = batch * draft
    rn, cn = lax.axis_size("row"), lax.axis_size("col")
    ri, ci = lax.axis_index("row"), lax.axis_index("col")
    core = ri & 1
    rmasks, cmasks = masks_of(rn), col_masks(cn)
    order = dest_order(cn, cmasks)
    place = jnp.array([order.index(d) for d in range(cn)], jnp.int32)[ci]
    groups = group_count.shape[0]
    hyper_width, slab, rank = gen_a.shape
    _, rank_part, ff = gen_b.shape

    per_dest = rows // cn
    step = per_dest // CHUNKS
    half = step // 2

    def arrange(x):
        x = x.reshape((cn, CHUNKS, 2, half) + x.shape[1:])
        x = jnp.concatenate([x[d : d + 1] for d in order])
        return x.transpose((1, 2, 0, 3) + tuple(range(4, x.ndim)))

    toks = arrange(tokens.reshape(rows, width)).reshape(CHUNKS, 2, cn * half, width)

    ends = jnp.cumsum(group_count)
    request = arrange(jnp.arange(rows, dtype=jnp.int32) // draft).reshape(CHUNKS, 2, cn * half)
    member = (request[..., None] >= (ends - group_count)) & (request[..., None] < ends)

    hyper = jax.nn.silu(
        jnp.dot(jnp.take(task_emb, group_task, axis=0), gen_in, preferred_element_type=F32)
    ).astype(BF16)

    a_local = jnp.dot(hyper, gen_a.reshape(hyper_width, slab * rank), preferred_element_type=F32)
    a_local = a_local.astype(BF16).reshape(groups, slab, rank).transpose(1, 0, 2)
    mine = lax.dynamic_slice_in_dim(toks, ci * slab, slab, 3).reshape(rows, slab)
    wide = jnp.dot(mine, a_local.reshape(slab, groups * rank), preferred_element_type=F32)
    low = jnp.sum(
        wide.reshape(rows, groups, rank) * member.reshape(rows, groups, 1).astype(F32), axis=1
    ).reshape(CHUNKS, 2, cn * half, rank)
    low = pick(low, core, 1) + swap(pick(low, 1 - core, 1), "row", 1)
    for m in rmasks[1:]:
        low = low + swap(low, "row", m)
    for m in cmasks:
        low = low + swap(low, "col", m)
    low = low.astype(BF16)
    low_mine = lax.dynamic_slice_in_dim(low, ri * rank_part, rank_part, 2)
    low_peer = lax.dynamic_slice_in_dim(low, (ri ^ 1) * rank_part, rank_part, 2)

    b_mine = jnp.dot(hyper, gen_b.reshape(hyper_width, rank_part * ff), preferred_element_type=F32)
    b_mine = b_mine.astype(BF16).reshape(groups * rank_part, ff)
    b_peer = swap(b_mine, "row", 1)

    own_member = pick(member, core, 1).astype(BF16)

    def spread(lowk, k):
        return (own_member[k][:, :, None] * lowk[k][:, None, :]).reshape(
            cn * half, groups * rank_part
        )

    keep, give = pick(toks, core, 1), pick(toks, 1 - core, 1)

    def partial(w, k):
        sent = jnp.dot(give[k], w, preferred_element_type=F32).astype(BF16)
        return jnp.dot(keep[k], w, preferred_element_type=F32) + swap(sent, "row", 1).astype(F32)

    def across(x):
        for m in rmasks[1:]:
            x = x + swap(x.astype(BF16), "row", m).astype(F32)
        return x

    gates = [across(partial(w_gate, k)) for k in range(CHUNKS)]
    ups = [partial(w_up, k) for k in range(CHUNKS)]
    outs = []
    for k in range(CHUNKS):
        up = (
            ups[k]
            + jnp.dot(spread(low_mine, k), b_mine, preferred_element_type=F32)
            + jnp.dot(spread(low_peer, k), b_peer, preferred_element_type=F32)
        )
        hid = (jax.nn.silu(gates[k]) * across(up)).astype(BF16)
        other = swap(hid, "row", 1)
        acc = jnp.stack(
            [
                jnp.dot(hid, w_down, preferred_element_type=F32),
                jnp.dot(other, w_down, preferred_element_type=F32),
            ]
        )
        out_width = acc.shape[-1]
        acc = acc.reshape((2,) + (2,) * len(cmasks) + (half, out_width))
        for s, m in enumerate(cmasks):
            dim = acc.ndim - 3
            bit = (place >> s) & 1
            sent = pick(acc, 1 - bit, dim).astype(BF16)
            acc = pick(acc, bit, dim) + swap(sent, "col", m).astype(F32)
        acc = acc.astype(BF16)
        outs.append(jnp.stack([pick(acc, core), pick(acc, 1 - core)]))
    out = jnp.stack(outs)
    return out.reshape(batch // cn, draft, out.shape[-1])


def solution(mesh):
    in_specs = (
        P(None, None, "row"),
        P(),
        P(),
        P(None, ("row", "col"), None),
        P(None, "row", "col"),
        P("row", "col"),
        P("row", "col"),
        P("col", "row"),
        P(),
        P(),
    )
    out_specs = P("col", None, "row")
    return jax.shard_map(shards, mesh=mesh, in_specs=in_specs, out_specs=out_specs, check_vma=False)
```

```python
import functools

import jax
import jax.numpy as jnp
import numpy as np
from jax import lax
from jax.experimental import pallas as pl
from jax.experimental.pallas import tpu as pltpu
from jax.sharding import PartitionSpec as P


F32 = jnp.float32
BF16 = jnp.bfloat16
CHUNKS = (1, 1)


def swap(x, axis, mask):
    n = lax.axis_size(axis)
    return lax.ppermute(x, axis, [(i, i ^ mask) for i in range(n)])


def masks_of(n):
    return [1 << b for b in range(n.bit_length() - 1)]


def pick(x, i, axis=0):
    return lax.dynamic_index_in_dim(x, i, axis, keepdims=False)


def stay(x):
    return pltpu.with_memory_space_constraint(x, pltpu.HBM)


def halves_of(n):
    return n // 2 if (n // 2) % 128 == 0 else n


def rows_of(tok_ref, request, size):
    draft, width = tok_ref.shape[1:]
    return tok_ref[pl.ds(request, size // draft)].reshape(size, width)


def split_store(x, w_ref, kept_ref, sent_ref, columns):
    half = x.shape[0] // 2
    both = jnp.dot(x, w_ref[:, columns], preferred_element_type=F32)
    kept_ref[:, columns] = both[:half]
    sent_ref[:, columns] = both[half:].astype(BF16)


def low_kernel(
    blocks, slab, shift, lead_ref, count_hbm, task_hbm, request_hbm, tok_hbm, emb_hbm, gen_in_hbm, a_hbm,
    w_hbm, *rest
):
    x_in, rest = (None, rest) if slab % 128 == 0 else (rest[0], rest[1:])
    low_ref, peer_ref, hyper_ref, member_ref, toks_ref, kept_ref, sent_ref = rest[:7]
    count_ref, task_ref, request_ref, tok_ref, emb_ref, gen_in_ref, a_ref, w_ref, ht_ref, sems = rest[7:]
    copies = [
        pltpu.make_async_copy(src, dst, sems.at[i])
        for i, (src, dst) in enumerate(
            (
                (task_hbm, task_ref),
                (count_hbm, count_ref),
                (request_hbm, request_ref),
                (emb_hbm, emb_ref),
                (gen_in_hbm, gen_in_ref),
                (tok_hbm, tok_ref),
                (a_hbm, a_ref),
                (w_hbm, w_ref),
            )
        )
    ]
    for copy in copies:
        copy.start()
    groups = count_ref.shape[1]
    tasks = emb_ref.shape[0]
    hidden = gen_in_ref.shape[1]
    rank, half = low_ref.shape
    rows = 2 * half
    core = lead_ref[1]
    across_rows = (((0,), (0,)), ((), ()))
    for copy in copies[:3]:
        copy.wait()
    chosen = lax.broadcasted_iota(jnp.int32, (tasks, groups), 0) == task_ref[...]
    chosen = chosen.astype(F32).astype(BF16)
    at = lax.broadcasted_iota(jnp.int32, (groups, groups), 0)
    of = lax.broadcasted_iota(jnp.int32, (groups, groups), 1)
    ends = jnp.sum(jnp.where(of <= at, count_ref[...], 0), axis=1, keepdims=True)
    starts = jnp.sum(jnp.where(of < at, count_ref[...], 0), axis=1, keepdims=True)
    first = lax.broadcasted_iota(jnp.int32, (1, rows), 1) < half
    request = request_ref[...] + shift * jnp.where(first, core, 1 - core)
    member = ((request >= starts) & (request < ends)).astype(F32).astype(BF16)
    member_ref[...] = member[:, :half]
    copies[3].wait()
    chosen = lax.dot_general(chosen, emb_ref[...], across_rows, preferred_element_type=F32)
    copies[4].wait()
    hyper = jnp.dot(chosen.astype(BF16), gen_in_ref[...], preferred_element_type=F32)
    hyper = (hyper * (1.0 / (1.0 + jnp.exp(-hyper)))).astype(BF16)
    hyper_ref[...] = hyper
    ht_ref[...] = lax.dot_general(hyper, member, across_rows, preferred_element_type=F32)
    copies[5].wait()
    for side in range(2):
        for source, target, size in blocks:
            begin = source + shift * (core if side == 0 else 1 - core)
            toks_ref[side * half + target : side * half + target + size, :] = rows_of(
                tok_ref, begin, size
            )
    x = toks_ref[:, pl.ds(pl.multiple_of(lead_ref[0], 128), slab)] if x_in is None else x_in[...]
    xt = x.T
    copies[6].wait()
    part = hidden // 4

    def body(i, acc):
        h = pl.multiple_of(i * part, part)
        t = jnp.dot(
            a_ref[pl.ds(pl.multiple_of(h * rank, part * rank), part * rank), :],
            xt,
            preferred_element_type=F32,
        ).reshape(part, rank, rows)
        return acc + jnp.sum(t * ht_ref[pl.ds(h, part), :][:, None, :], axis=0)

    low = lax.fori_loop(0, hidden // part, body, jnp.zeros((rank, rows), F32))
    low_ref[...] = low[:, :half]
    peer_ref[...] = low[:, half:]
    copies[7].wait()
    ff = w_ref.shape[1]
    tile = halves_of(ff)
    for j in range(0, ff, tile):
        split_store(toks_ref[...], w_ref, kept_ref, sent_ref, slice(j, j + tile))


def low_part(blocks, shift, lead, count, task, request, tokens, emb, gen_in, a, w, x):
    hidden, slab, rank = a.shape
    groups, rows = count.shape[1], request.shape[1]
    width, ff = w.shape
    a = a.transpose(0, 2, 1).reshape(hidden * rank, slab)
    vmem = pl.BlockSpec(memory_space=pltpu.VMEM)
    hbm = pl.BlockSpec(memory_space=pltpu.HBM)
    moved = (count, task, request, tokens, emb, gen_in, a, w)
    extra = () if x is None else (x,)
    return pl.pallas_call(
        functools.partial(low_kernel, blocks, slab, shift),
        in_specs=[pl.BlockSpec(memory_space=pltpu.SMEM)] + [hbm] * len(moved) + [vmem] * len(extra),
        out_specs=[vmem] * 7,
        out_shape=(
            jax.ShapeDtypeStruct((rank, rows // 2), F32),
            jax.ShapeDtypeStruct((rank, rows // 2), F32),
            jax.ShapeDtypeStruct((groups, hidden), BF16),
            jax.ShapeDtypeStruct((groups, rows // 2), BF16),
            jax.ShapeDtypeStruct((rows, width), BF16),
            jax.ShapeDtypeStruct((rows // 2, ff), F32),
            jax.ShapeDtypeStruct((rows // 2, ff), BF16),
        ),
        scratch_shapes=[pltpu.VMEM(m.shape, m.dtype) for m in moved]
        + [pltpu.VMEM((hidden, rows), F32), pltpu.SemaphoreType.DMA((len(moved),))],
        compiler_params=pltpu.CompilerParams(vmem_limit_bytes=36 << 20),
        name="low_part",
    )(lead, *[stay(m) for m in moved], *extra)


def split_kernel(x_ref, w_ref, kept_ref, sent_ref):
    split_store(x_ref[...], w_ref, kept_ref, sent_ref, slice(None))


def split_matmul(x, w):
    rows, width = x.shape
    ff = w.shape[1]
    tile = halves_of(ff)
    return pl.pallas_call(
        split_kernel,
        grid=(ff // tile,),
        in_specs=[
            pl.BlockSpec((rows, width), lambda i: (0, 0)),
            pl.BlockSpec((width, tile), lambda i: (0, i)),
        ],
        out_specs=[
            pl.BlockSpec((rows // 2, tile), lambda i: (0, i)),
            pl.BlockSpec((rows // 2, tile), lambda i: (0, i)),
        ],
        out_shape=(
            pltpu.HBM((rows // 2, ff), F32),
            jax.ShapeDtypeStruct((rows // 2, ff), BF16),
        ),
        compiler_params=pltpu.CompilerParams(vmem_limit_bytes=16 << 20),
    )(x, w)


def factor_kernel(hyper_ref, gen_ref, out_ref, wide_ref):
    hidden, ranks, tile = gen_ref.shape
    groups = hyper_ref.shape[0]

    @pl.when(pl.program_id(0) == 0)
    def _():
        part = 128
        spread = part * ranks
        lane = lax.broadcasted_iota(jnp.int32, (part, spread), 1)
        first = lax.broadcasted_iota(jnp.int32, (part, spread), 0) * ranks
        repeat = ((lane >= first) & (lane < first + ranks)).astype(F32).astype(BF16)
        which = lax.rem(lax.broadcasted_iota(jnp.int32, (groups, spread), 1), ranks)
        for k in range(hidden // part):
            wide = jnp.dot(
                hyper_ref[:, k * part : (k + 1) * part], repeat, preferred_element_type=F32
            )
            for r in range(ranks):
                wide_ref[r * groups : (r + 1) * groups, k * spread : (k + 1) * spread] = jnp.where(
                    which == r, wide, 0.0
                ).astype(BF16)

    out_ref[...] = jnp.dot(
        wide_ref[...], gen_ref[...].reshape(hidden * ranks, tile), preferred_element_type=F32
    ).astype(BF16)


def factors(hyper, gen_b):
    hidden, ranks, ff = gen_b.shape
    groups = hyper.shape[0]
    tile = halves_of(ff)
    return pl.pallas_call(
        factor_kernel,
        grid=(ff // tile,),
        in_specs=[
            pl.BlockSpec((groups, hidden), lambda i: (0, 0)),
            pl.BlockSpec((hidden, ranks, tile), lambda i: (0, 0, i)),
        ],
        out_specs=pl.BlockSpec((ranks * groups, tile), lambda i: (0, i)),
        out_shape=jax.ShapeDtypeStruct((ranks * groups, ff), BF16),
        scratch_shapes=[pltpu.VMEM((ranks * groups, hidden * ranks), BF16)],
        compiler_params=pltpu.CompilerParams(vmem_limit_bytes=24 << 20),
        name="factors",
    )(hyper, gen_b)


def delta_kernel(pieces, rank_ref, low_ref, member_ref, mine_ref, peer_ref, kept_ref, got_ref, sum_ref, *sent):
    groups = member_ref.shape[0]
    ranks = mine_ref.shape[0] // groups
    member = member_ref[...].astype(F32)
    total = kept_ref[...] + got_ref[...].astype(F32)
    for which, factor in ((0, mine_ref), (1, peer_ref)):
        first = rank_ref[which]
        spread = jnp.concatenate(
            [
                (member * low_ref[pl.ds(first + r, 1), :].astype(BF16).astype(F32)).astype(BF16)
                for r in range(ranks)
            ],
            axis=0,
        )
        total += lax.dot_general(
            spread, factor[...], (((0,), (0,)), ((), ())), preferred_element_type=F32
        )
    sum_ref[...] = total
    total = total.astype(BF16)
    for (start, size), ref in zip(pieces, sent):
        ref[...] = total[start : start + size]


def add_adapter(pieces, first_ranks, low, member, mine, peer, kept, got):
    rows, ff = kept.shape
    tile = halves_of(ff)
    whole = lambda x: pl.BlockSpec(x.shape, lambda i, c: (0, 0))
    cut = lambda n: pl.BlockSpec((n, tile), lambda i, c: (0, i))
    return pl.pallas_call(
        functools.partial(delta_kernel, pieces),
        grid_spec=pltpu.PrefetchScalarGridSpec(
            num_scalar_prefetch=1,
            grid=(ff // tile,),
            in_specs=[whole(low), whole(member)] + [cut(x.shape[0]) for x in (mine, peer, kept, got)],
            out_specs=[cut(rows)] + [cut(size) for _, size in pieces],
        ),
        out_shape=[pltpu.VMEM((rows, ff), F32)]
        + [jax.ShapeDtypeStruct((size, ff), BF16) for _, size in pieces],
        compiler_params=pltpu.CompilerParams(vmem_limit_bytes=16 << 20),
        name="adapter",
    )(first_ranks, low, member, mine, peer, stay(kept), got)


def gate_kernel(kept_ref, core_ref, rest_ref, later_ref, out_ref):
    gate = kept_ref[...] + core_ref[...].astype(F32) + rest_ref[...].astype(F32)
    out_ref[...] = gate * (1.0 / (1.0 + jnp.exp(-gate)))


def activate(kept, core_got, rest, later):
    return in_vmem(gate_kernel, pltpu.VMEM(kept.shape, F32), kept, core_got, rest, later)


def in_vmem(kernel, out, *args):
    vmem = pl.BlockSpec(memory_space=pltpu.VMEM)
    return pl.pallas_call(
        kernel,
        in_specs=[vmem] * len(args),
        out_specs=vmem,
        out_shape=out,
        compiler_params=pltpu.CompilerParams(vmem_limit_bytes=8 << 20),
    )(*args)


def hidden_kernel(start, act_ref, half_ref, up_ref, out_ref):
    at = slice(start, start + out_ref.shape[0])
    out_ref[...] = (act_ref[at] * (half_ref[at] + up_ref[...].astype(F32))).astype(BF16)


def hidden_units(piece, act, half, up_got):
    start, size = piece
    out = jax.ShapeDtypeStruct((size, act.shape[1]), BF16)
    return in_vmem(functools.partial(hidden_kernel, start), out, act, half, up_got)


def shards(tokens, task_emb, gen_in, gen_a, gen_b, w_gate, w_up, w_down, group_count, group_task):
    batch, draft, _ = tokens.shape
    rows = batch * draft
    rn, cn = lax.axis_size("row"), lax.axis_size("col")
    ri, ci = lax.axis_index("row"), lax.axis_index("col")
    core = ri & 1
    rmasks, cmasks = masks_of(rn), masks_of(cn)
    slab = gen_a.shape[1]
    rank_part, _ = gen_b.shape[1:]

    per_dest = rows // cn
    sizes = [per_dest * part // sum(CHUNKS) for part in CHUNKS]
    blocks, pieces, target, source = [], [], 0, 0
    for size in sizes:
        pieces.append((target, cn * size // 2))
        for d in range(cn):
            blocks.append(((d * per_dest + source) // draft, target, size // 2))
            target += size // 2
        source += size // 2
    shift = per_dest // 2 // draft

    request = np.concatenate([begin + np.arange(size) // draft for begin, _, size in blocks])
    request = np.concatenate([request, request])[None, :].astype(np.int32)
    x = None
    if slab % 128:
        x = lax.dynamic_slice_in_dim(tokens, ci * slab, slab, 2)
        x = jnp.concatenate(
            [
                lax.dynamic_slice_in_dim(x, begin + shift * side, size // draft).reshape(size, slab)
                for side in (core, 1 - core)
                for begin, _, size in blocks
            ]
        )
    low, low_sent, hyper, own_member, toks, gate_kept, gate_sent = low_part(
        tuple(blocks),
        shift,
        jnp.stack([ci * slab, core]),
        group_count[None, :],
        group_task[None, :],
        jnp.asarray(request),
        tokens,
        task_emb,
        gen_in,
        gen_a,
        w_gate,
        x,
    )
    low = low + swap(low_sent, "row", 1)
    gate_got = swap(gate_sent, "row", 1)
    for m in rmasks[1:]:
        low = low + swap(low, "row", m)
    gate_sum = (gate_kept + gate_got.astype(F32)).astype(BF16)

    def others(sent):
        total = None
        for s, m in enumerate(rmasks[1:]):
            got = swap(sent, "row", m)
            if s + 2 == len(rmasks) and total is None:
                return got
            total = got.astype(F32) if total is None else total + got.astype(F32)
            sent = (sent.astype(F32) + got.astype(F32)).astype(BF16)
        return total

    gate_rest = others(gate_sum)

    up_kept, up_sent = split_matmul(toks, w_up)
    up_got = swap(up_sent, "row", 1)
    b_mine = factors(hyper, gen_b)
    b_peer = swap(b_mine, "row", 1)
    for m in cmasks:
        low = low + swap(low, "col", m)

    first_ranks = jnp.stack([ri * rank_part, (ri ^ 1) * rank_part])
    up_half, *up_sums = add_adapter(
        tuple(pieces), first_ranks, low, own_member, b_mine, b_peer, up_kept, up_got
    )

    act = activate(gate_kept, gate_got, gate_rest, w_down)
    outs = []
    for k, piece in enumerate(pieces):
        up_rest = others(up_sums[k])
        hid = hidden_units(piece, act, up_half, up_rest)
        other = swap(hid, "row", 1)
        acc = jnp.dot(hid, w_down, preferred_element_type=F32)
        acc = jnp.stack([acc, jnp.dot(other, w_down, preferred_element_type=F32)])
        out_width = acc.shape[-1]
        acc = acc.reshape((2,) + (2,) * len(cmasks) + (sizes[k] // 2, out_width))
        for s, m in enumerate(cmasks):
            dim = acc.ndim - 3
            bit = (ci >> s) & 1
            sent = pick(acc, 1 - bit, dim).astype(BF16)
            acc = pick(acc, bit, dim) + swap(sent, "col", m).astype(F32)
        acc = acc.astype(BF16)
        outs.append(jnp.stack([pick(acc, core), pick(acc, 1 - core)]))
    out = jnp.concatenate(outs, axis=1)
    return out.reshape(batch // cn, draft, out.shape[-1])


def solution(mesh):
    in_specs = (
        P(None, None, "row"),
        P(),
        P(),
        P(None, ("row", "col"), None),
        P(None, "row", "col"),
        P("row", "col"),
        P("row", "col"),
        P("col", "row"),
        P(),
        P(),
    )
    out_specs = P("col", None, "row")

    return jax.shard_map(shards, mesh=mesh, in_specs=in_specs, out_specs=out_specs, check_vma=False)
```

```python
import functools

import jax
import jax.numpy as jnp
import numpy as np
from jax import lax
from jax.experimental import pallas as pl
from jax.experimental.pallas import tpu as pltpu
from jax.sharding import PartitionSpec as P


F32 = jnp.float32
BF16 = jnp.bfloat16


def plan(per_dest):
    if per_dest % 64 == 0:
        return (2, 1, 1), ((0, 1), (2,))
    return (1, 1), ((0,), (1,))


def swap(x, axis, mask):
    n = lax.axis_size(axis)
    return lax.ppermute(x, axis, [(i, i ^ mask) for i in range(n)])


def masks_of(n):
    return [1 << b for b in range(n.bit_length() - 1)]


def stay(x):
    return pltpu.with_memory_space_constraint(x, pltpu.HBM)


def halves_of(n):
    return n // 2 if (n // 2) % 128 == 0 else n


def rows_of(tok_ref, request, size):
    draft, width = tok_ref.shape[1:]
    return tok_ref[pl.ds(request, size // draft)].reshape(size, width)


def split_store(x, w_ref, kept_ref, sent_ref, columns):
    half = x.shape[0] // 2
    both = jnp.dot(x, w_ref[:, columns], preferred_element_type=F32)
    kept_ref[:, columns] = both[:half]
    sent_ref[:, columns] = both[half:].astype(BF16)


def low_kernel(
    blocks, slab, shift, count_hbm, task_hbm, request_hbm, tok_hbm, emb_hbm, gen_in_hbm, a_hbm,
    w_hbm, *rest
):
    x_in, rest = (None, rest) if slab % 128 == 0 else (rest[0], rest[1:])
    low_ref, peer_ref, hyper_ref, member_ref, toks_ref, kept_ref, sent_ref = rest[:7]
    count_ref, task_ref, request_ref, tok_ref, emb_ref, gen_in_ref, a_ref, w_ref, ht_ref, sems = rest[7:]
    copies = [
        pltpu.make_async_copy(src, dst, sems.at[i])
        for i, (src, dst) in enumerate(
            (
                (task_hbm, task_ref),
                (count_hbm, count_ref),
                (request_hbm, request_ref),
                (emb_hbm, emb_ref),
                (gen_in_hbm, gen_in_ref),
                (tok_hbm, tok_ref),
                (a_hbm, a_ref),
                (w_hbm, w_ref),
            )
        )
    ]
    for copy in copies:
        copy.start()
    groups = count_ref.shape[1]
    tasks = emb_ref.shape[0]
    hidden = gen_in_ref.shape[1]
    rank, half = low_ref.shape
    rows = 2 * half
    core = lax.axis_index("row") & 1
    across_rows = (((0,), (0,)), ((), ()))
    for copy in copies[:3]:
        copy.wait()
    chosen = lax.broadcasted_iota(jnp.int32, (tasks, groups), 0) == task_ref[...]
    chosen = chosen.astype(F32).astype(BF16)
    at = lax.broadcasted_iota(jnp.int32, (groups, groups), 0)
    of = lax.broadcasted_iota(jnp.int32, (groups, groups), 1)
    ends = jnp.sum(jnp.where(of <= at, count_ref[...], 0), axis=1, keepdims=True)
    starts = jnp.sum(jnp.where(of < at, count_ref[...], 0), axis=1, keepdims=True)
    first = lax.broadcasted_iota(jnp.int32, (1, rows), 1) < half
    request = request_ref[...] + shift * jnp.where(first, core, 1 - core)
    member = ((request >= starts) & (request < ends)).astype(F32).astype(BF16)
    member_ref[...] = member[:, :half]
    copies[3].wait()
    chosen = lax.dot_general(chosen, emb_ref[...], across_rows, preferred_element_type=F32)
    copies[4].wait()
    hyper = jnp.dot(chosen.astype(BF16), gen_in_ref[...], preferred_element_type=F32)
    hyper = (hyper * (1.0 / (1.0 + jnp.exp(-hyper)))).astype(BF16)
    hyper_ref[...] = hyper
    ht_ref[...] = lax.dot_general(hyper, member, across_rows, preferred_element_type=F32)
    copies[5].wait()
    for side in range(2):
        for source, target, size in blocks:
            begin = source + shift * (core if side == 0 else 1 - core)
            toks_ref[side * half + target : side * half + target + size, :] = rows_of(
                tok_ref, begin, size
            )
    x = toks_ref[:, pl.ds(pl.multiple_of(lax.axis_index("col") * slab, 128), slab)] if x_in is None else x_in[...]
    xt = x.T
    copies[6].wait()
    part = hidden // 4

    def body(i, acc):
        h = pl.multiple_of(i * part, part)
        t = jnp.dot(
            a_ref[pl.ds(pl.multiple_of(h * rank, part * rank), part * rank), :],
            xt,
            preferred_element_type=F32,
        ).reshape(part, rank, rows)
        return acc + jnp.sum(t * ht_ref[pl.ds(h, part), :][:, None, :], axis=0)

    low = lax.fori_loop(0, hidden // part, body, jnp.zeros((rank, rows), F32))
    low_ref[...] = low[:, :half]
    peer_ref[...] = low[:, half:]
    copies[7].wait()
    ff = w_ref.shape[1]
    tile = halves_of(ff)
    for j in range(0, ff, tile):
        split_store(toks_ref[...], w_ref, kept_ref, sent_ref, slice(j, j + tile))


def low_part(blocks, shift, count, task, request, tokens, emb, gen_in, a, w, x):
    hidden, slab, rank = a.shape
    groups, rows = count.shape[1], request.shape[1]
    width, ff = w.shape
    a = a.transpose(0, 2, 1).reshape(hidden * rank, slab)
    vmem = pl.BlockSpec(memory_space=pltpu.VMEM)
    hbm = pl.BlockSpec(memory_space=pltpu.HBM)
    moved = (count, task, request, tokens, emb, gen_in, a, w)
    extra = () if x is None else (x,)
    return pl.pallas_call(
        functools.partial(low_kernel, blocks, slab, shift),
        in_specs=[hbm] * len(moved) + [vmem] * len(extra),
        out_specs=[vmem] * 7,
        out_shape=(
            jax.ShapeDtypeStruct((rank, rows // 2), F32),
            jax.ShapeDtypeStruct((rank, rows // 2), F32),
            jax.ShapeDtypeStruct((groups, hidden), BF16),
            jax.ShapeDtypeStruct((groups, rows // 2), BF16),
            jax.ShapeDtypeStruct((rows, width), BF16),
            jax.ShapeDtypeStruct((rows // 2, ff), F32),
            jax.ShapeDtypeStruct((rows // 2, ff), BF16),
        ),
        scratch_shapes=[pltpu.VMEM(m.shape, m.dtype) for m in moved]
        + [pltpu.VMEM((hidden, rows), F32), pltpu.SemaphoreType.DMA((len(moved),))],
        compiler_params=pltpu.CompilerParams(vmem_limit_bytes=36 << 20),
        name="low_part",
    )(*[stay(m) for m in moved], *extra)


def split_kernel(x_ref, w_ref, kept_ref, sent_ref):
    split_store(x_ref[...], w_ref, kept_ref, sent_ref, slice(None))


def split_matmul(x, w):
    rows, width = x.shape
    ff = w.shape[1]
    tile = halves_of(ff)
    return pl.pallas_call(
        split_kernel,
        grid=(ff // tile,),
        in_specs=[
            pl.BlockSpec((rows, width), lambda i: (0, 0)),
            pl.BlockSpec((width, tile), lambda i: (0, i)),
        ],
        out_specs=[
            pl.BlockSpec((rows // 2, tile), lambda i: (0, i)),
            pl.BlockSpec((rows // 2, tile), lambda i: (0, i)),
        ],
        out_shape=(
            pltpu.VMEM((rows // 2, ff), F32),
            jax.ShapeDtypeStruct((rows // 2, ff), BF16),
        ),
        compiler_params=pltpu.CompilerParams(vmem_limit_bytes=16 << 20),
    )(x, w)


def factor_kernel(hyper_ref, gen_ref, out_ref, wide_ref):
    hidden, ranks, tile = gen_ref.shape
    groups = hyper_ref.shape[0]

    @pl.when(pl.program_id(0) == 0)
    def _():
        part = 128
        spread = part * ranks
        lane = lax.broadcasted_iota(jnp.int32, (part, spread), 1)
        first = lax.broadcasted_iota(jnp.int32, (part, spread), 0) * ranks
        repeat = ((lane >= first) & (lane < first + ranks)).astype(F32).astype(BF16)
        which = lax.rem(lax.broadcasted_iota(jnp.int32, (groups, spread), 1), ranks)
        for k in range(hidden // part):
            wide = jnp.dot(
                hyper_ref[:, k * part : (k + 1) * part], repeat, preferred_element_type=F32
            )
            for r in range(ranks):
                wide_ref[r * groups : (r + 1) * groups, k * spread : (k + 1) * spread] = jnp.where(
                    which == r, wide, 0.0
                ).astype(BF16)

    out_ref[...] = jnp.dot(
        wide_ref[...], gen_ref[...].reshape(hidden * ranks, tile), preferred_element_type=F32
    ).astype(BF16)


def factors(hyper, gen_b):
    hidden, ranks, ff = gen_b.shape
    groups = hyper.shape[0]
    tile = halves_of(ff)
    return pl.pallas_call(
        factor_kernel,
        grid=(ff // tile,),
        in_specs=[
            pl.BlockSpec((groups, hidden), lambda i: (0, 0)),
            pl.BlockSpec((hidden, ranks, tile), lambda i: (0, 0, i)),
        ],
        out_specs=pl.BlockSpec((ranks * groups, tile), lambda i: (0, i)),
        out_shape=jax.ShapeDtypeStruct((ranks * groups, ff), BF16),
        scratch_shapes=[pltpu.VMEM((ranks * groups, hidden * ranks), BF16)],
        compiler_params=pltpu.CompilerParams(vmem_limit_bytes=24 << 20),
        name="factors",
    )(hyper, gen_b)


def delta_kernel(pieces, low_ref, member_ref, mine_ref, peer_ref, kept_ref, got_ref, sum_ref, *sent):
    groups = member_ref.shape[0]
    ranks = mine_ref.shape[0] // groups
    member = member_ref[...].astype(F32)
    total = kept_ref[...] + got_ref[...].astype(F32)
    for which, factor in ((0, mine_ref), (1, peer_ref)):
        first = (lax.axis_index("row") ^ which) * ranks
        spread = jnp.concatenate(
            [
                (member * low_ref[pl.ds(first + r, 1), :].astype(BF16).astype(F32)).astype(BF16)
                for r in range(ranks)
            ],
            axis=0,
        )
        total += lax.dot_general(
            spread, factor[...], (((0,), (0,)), ((), ())), preferred_element_type=F32
        )
    sum_ref[...] = total
    total = total.astype(BF16)
    for (start, size), ref in zip(pieces, sent):
        ref[...] = total[start : start + size]


def add_adapter(pieces, low, member, mine, peer, kept, got):
    rows, ff = kept.shape
    tile = halves_of(ff)
    whole = lambda x: pl.BlockSpec(x.shape, lambda i: (0, 0))
    cut = lambda n: pl.BlockSpec((n, tile), lambda i: (0, i))
    return pl.pallas_call(
        functools.partial(delta_kernel, pieces),
        grid=(ff // tile,),
        in_specs=[whole(low), whole(member)] + [cut(x.shape[0]) for x in (mine, peer, kept, got)],
        out_specs=[cut(rows)] + [cut(size) for _, size in pieces],
        out_shape=[pltpu.VMEM((rows, ff), F32)]
        + [jax.ShapeDtypeStruct((size, ff), BF16) for _, size in pieces],
        compiler_params=pltpu.CompilerParams(vmem_limit_bytes=16 << 20),
        name="adapter",
    )(low, member, mine, peer, kept, got)


def gate_kernel(kept_ref, core_ref, rest_ref, later_ref, out_ref):
    gate = kept_ref[...] + core_ref[...].astype(F32) + rest_ref[...].astype(F32)
    out_ref[...] = gate * (1.0 / (1.0 + jnp.exp(-gate)))


def activate(kept, core_got, rest, later):
    return in_vmem(gate_kernel, pltpu.VMEM(kept.shape, F32), kept, core_got, rest, later)


def in_vmem(kernel, out, *args):
    vmem = pl.BlockSpec(memory_space=pltpu.VMEM)
    return pl.pallas_call(
        kernel,
        in_specs=[vmem] * len(args),
        out_specs=jax.tree.map(lambda _: vmem, out),
        out_shape=out,
        compiler_params=pltpu.CompilerParams(vmem_limit_bytes=8 << 20),
    )(*args)


def split_rows(hid_ref, w_ref):
    acc = jnp.dot(hid_ref[...], w_ref[...], preferred_element_type=F32)
    col = lax.axis_size("col")
    acc = acc.reshape(col // 2, 2, acc.shape[0] // col, acc.shape[1])
    low_bit = (lax.axis_index("col") & 1) == 0
    keep = jnp.where(low_bit, acc[:, 0], acc[:, 1])
    give = jnp.where(low_bit, acc[:, 1], acc[:, 0])
    return keep, give.astype(BF16)


def down_kernel(hid_ref, w_ref, keep_ref, give_ref):
    keep_ref[...], give_ref[...] = split_rows(hid_ref, w_ref)


def cross_kernel(hid_ref, w_ref, own_keep_ref, own_give_ref, keep_ref, give_ref):
    keep_ref[0], give_ref[0] = own_keep_ref[...], own_give_ref[...]
    keep_ref[1], give_ref[1] = split_rows(hid_ref, w_ref)


def down(hid, w):
    col = lax.axis_size("col")
    shape = (col // 2, hid.shape[0] // col, w.shape[1])
    out = (jax.ShapeDtypeStruct(shape, F32), jax.ShapeDtypeStruct(shape, BF16))
    return in_vmem(down_kernel, out, hid, w)


def cross(other, w, own):
    out = tuple(jax.ShapeDtypeStruct((2,) + x.shape, x.dtype) for x in own)
    return in_vmem(cross_kernel, out, other, w, *own)


def fold_kernel(bit, keep_ref, got_ref, new_ref, give_ref):
    parts = keep_ref.shape[1]
    side = (lax.axis_index("col") >> bit) & 1
    for j in range(parts // 2):
        for ref, which in ((new_ref, side), (give_ref, 1 - side)):
            at = pl.ds(2 * j + which, 1)
            ref[:, j : j + 1] = (keep_ref[:, at] + got_ref[:, at].astype(F32)).astype(ref.dtype)


def fold(bit, keep, got):
    shape = keep.shape[:1] + (keep.shape[1] // 2,) + keep.shape[2:]
    out = (jax.ShapeDtypeStruct(shape, F32), jax.ShapeDtypeStruct(shape, BF16))
    return in_vmem(functools.partial(fold_kernel, bit), out, keep, got)


def last_kernel(bit, count, *refs):
    here = lax.axis_index("col") >> bit
    start = 0
    for k in range(count):
        keep_ref, got_ref = refs[2 * k : 2 * k + 2]
        rows = slice(start, start + keep_ref.shape[2])
        for q, ref in enumerate(refs[2 * count :]):
            at = pl.ds(here ^ q, 1)
            ref[:, :, rows] = (keep_ref[:, at] + got_ref[:, at].astype(F32)).astype(ref.dtype)
        start = rows.stop


def last_split(bit, parts):
    keep = parts[0][0]
    shape = keep.shape[:1] + (1, sum(k.shape[2] for k, _ in parts)) + keep.shape[3:]
    out = [jax.ShapeDtypeStruct(shape, F32)] + [jax.ShapeDtypeStruct(shape, BF16)] * 3
    kernel = functools.partial(last_kernel, bit, len(parts))
    return in_vmem(kernel, out, *[x for part in parts for x in part])


def join_kernel(count, *refs):
    out_ref = refs[-1]
    requests, draft, width = out_ref.shape
    core = lax.axis_index("row") & 1
    start = 0
    for k in range(count):
        total, *got = refs[4 * k : 4 * k + 4]
        for side in range(2):
            value = total[side, 0]
            for g in got:
                value += g[side, 0].astype(F32)
            size = value.shape[0] // draft
            at = start + (requests // 2) * (core if side == 0 else 1 - core)
            out_ref[pl.ds(at, size)] = value.astype(BF16).reshape(size, draft, width)
        start += size


def join(parts, out):
    return in_vmem(functools.partial(join_kernel, len(parts)), out, *[x for p in parts for x in p])


def hidden_kernel(start, act_ref, half_ref, up_ref, out_ref):
    at = slice(start, start + out_ref.shape[0])
    out_ref[...] = (act_ref[at] * (half_ref[at] + up_ref[...].astype(F32))).astype(BF16)


def hidden_units(piece, act, half, up_got):
    start, size = piece
    out = jax.ShapeDtypeStruct((size, act.shape[1]), BF16)
    return in_vmem(functools.partial(hidden_kernel, start), out, act, half, up_got)


def shards(tokens, task_emb, gen_in, gen_a, gen_b, w_gate, w_up, w_down, group_count, group_task):
    batch, draft, _ = tokens.shape
    rows = batch * draft
    rn, cn = lax.axis_size("row"), lax.axis_size("col")
    ri, ci = lax.axis_index("row"), lax.axis_index("col")
    core = ri & 1
    rmasks, cmasks = masks_of(rn), masks_of(cn)
    slab = gen_a.shape[1]

    per_dest = rows // cn
    chunks, joint = plan(per_dest)
    sizes = [per_dest * part // sum(chunks) for part in chunks]
    blocks, pieces, target, source = [], [], 0, 0
    for size in sizes:
        pieces.append((target, cn * size // 2))
        for d in range(cn):
            blocks.append(((d * per_dest + source) // draft, target, size // 2))
            target += size // 2
        source += size // 2
    shift = per_dest // 2 // draft

    request = np.concatenate([begin + np.arange(size) // draft for begin, _, size in blocks])
    request = np.concatenate([request, request])[None, :].astype(np.int32)
    x = None
    if slab % 128:
        x = lax.dynamic_slice_in_dim(tokens, ci * slab, slab, 2)
        x = jnp.concatenate(
            [
                lax.dynamic_slice_in_dim(x, begin + shift * side, size // draft).reshape(size, slab)
                for side in (core, 1 - core)
                for begin, _, size in blocks
            ]
        )
    low, low_sent, hyper, own_member, toks, gate_kept, gate_sent = low_part(
        tuple(blocks),
        shift,
        group_count[None, :],
        group_task[None, :],
        jnp.asarray(request),
        tokens,
        task_emb,
        gen_in,
        gen_a,
        w_gate,
        x,
    )
    low = low + swap(low_sent, "row", 1)
    gate_got = swap(gate_sent, "row", 1)
    for m in rmasks[1:]:
        low = low + swap(low, "row", m)
    gate_sum = (gate_kept + gate_got.astype(F32)).astype(BF16)

    def others(sent):
        total = None
        for s, m in enumerate(rmasks[1:]):
            got = swap(sent, "row", m)
            if s + 2 == len(rmasks) and total is None:
                return got
            total = got.astype(F32) if total is None else total + got.astype(F32)
            sent = (sent.astype(F32) + got.astype(F32)).astype(BF16)
        return total

    gate_rest = others(gate_sum)

    up_kept, up_sent = split_matmul(toks, w_up)
    up_got = swap(up_sent, "row", 1)
    b_mine = factors(hyper, gen_b)
    b_peer = swap(b_mine, "row", 1)
    for m in cmasks:
        low = low + swap(low, "col", m)

    up_half, *up_sums = add_adapter(
        tuple(pieces), low, own_member, b_mine, b_peer, up_kept, up_got
    )

    act = activate(gate_kept, gate_got, gate_rest, w_down)
    outs = []
    for k, piece in enumerate(pieces):
        up_rest = others(up_sums[k])
        hid = hidden_units(piece, act, up_half, up_rest)
        other = swap(hid, "row", 1)
        keep, give = cross(other, w_down, down(hid, w_down))
        for s, m in enumerate(cmasks[:-2]):
            got = swap(give, "col", m)
            if s + 3 < len(cmasks):
                keep, give = fold(s + 1, keep, got)
        outs.append((keep, got))
    low_bit = len(cmasks) - 2
    parts = []
    for members in joint:
        total, *gives = last_split(low_bit, [outs[k] for k in members])
        gots = [swap(give, "col", (q + 1) << low_bit) for q, give in enumerate(gives)]
        parts.append([total] + gots)
    return join(parts, jax.ShapeDtypeStruct((batch // cn, draft, w_down.shape[1]), BF16))


def solution(mesh):
    in_specs = (
        P(None, None, "row"),
        P(),
        P(),
        P(None, ("row", "col"), None),
        P(None, "row", "col"),
        P("row", "col"),
        P("row", "col"),
        P("col", "row"),
        P(),
        P(),
    )
    out_specs = P("col", None, "row")

    return jax.shard_map(shards, mesh=mesh, in_specs=in_specs, out_specs=out_specs, check_vma=False)
```

```python
import functools

import jax
import jax.numpy as jnp
import numpy as np
from jax import lax
from jax.experimental import pallas as pl
from jax.experimental.pallas import tpu as pltpu
from jax.sharding import PartitionSpec as P


F32 = jnp.float32
BF16 = jnp.bfloat16


def plan(per_dest):
    if per_dest % 64 == 0:
        return (1, 1, 1, 1), ((1, 2), (3,)), True
    return (1, 1), ((0,), (1,)), False


def swap(x, axis, mask):
    n = lax.axis_size(axis)
    return lax.ppermute(x, axis, [(i, i ^ mask) for i in range(n)])


def masks_of(n):
    return [1 << b for b in range(n.bit_length() - 1)]


def stay(x):
    return pltpu.with_memory_space_constraint(x, pltpu.HBM)


def halves_of(n):
    return n // 2 if (n // 2) % 128 == 0 else n


def rows_of(tok_ref, request, size):
    draft, width = tok_ref.shape[1:]
    return tok_ref[pl.ds(request, size // draft)].reshape(size, width)


def split_store(x, w_ref, kept_ref, sent_ref, columns):
    half = x.shape[0] // 2
    both = jnp.dot(x, w_ref[:, columns], preferred_element_type=F32)
    kept_ref[:, columns] = both[:half]
    sent_ref[:, columns] = both[half:].astype(BF16)


def low_kernel(
    blocks, slab, shift, count_hbm, task_hbm, request_hbm, tok_hbm, emb_hbm, gen_in_hbm, a_hbm,
    w_hbm, *rest
):
    x_in, rest = (None, rest) if slab % 128 == 0 else (rest[0], rest[1:])
    low_ref, hyper_ref, member_ref, toks_ref, kept_ref, sent_ref = rest[:6]
    count_ref, task_ref, request_ref, tok_ref, emb_ref, gen_in_ref, a_ref, w_ref, ht_ref, sems = rest[6:]
    copies = [
        pltpu.make_async_copy(src, dst, sems.at[i])
        for i, (src, dst) in enumerate(
            (
                (task_hbm, task_ref),
                (count_hbm, count_ref),
                (request_hbm, request_ref),
                (emb_hbm, emb_ref),
                (gen_in_hbm, gen_in_ref),
                (tok_hbm, tok_ref),
                (a_hbm, a_ref),
                (w_hbm, w_ref),
            )
        )
    ]
    for copy in copies:
        copy.start()
    groups = count_ref.shape[1]
    tasks = emb_ref.shape[0]
    hidden = gen_in_ref.shape[1]
    rank, rows = low_ref.shape
    half = rows // 2
    core = lax.axis_index("row") & 1
    across_rows = (((0,), (0,)), ((), ()))
    for copy in copies[:3]:
        copy.wait()
    chosen = lax.broadcasted_iota(jnp.int32, (tasks, groups), 0) == task_ref[...]
    chosen = chosen.astype(F32).astype(BF16)
    at = lax.broadcasted_iota(jnp.int32, (groups, groups), 0)
    of = lax.broadcasted_iota(jnp.int32, (groups, groups), 1)
    ends = jnp.sum(jnp.where(of <= at, count_ref[...], 0), axis=1, keepdims=True)
    starts = jnp.sum(jnp.where(of < at, count_ref[...], 0), axis=1, keepdims=True)
    first = lax.broadcasted_iota(jnp.int32, (1, rows), 1) < half
    request = request_ref[...] + shift * jnp.where(first, core, 1 - core)
    member = ((request >= starts) & (request < ends)).astype(F32).astype(BF16)
    member_ref[...] = member[:, :half]
    copies[3].wait()
    chosen = lax.dot_general(chosen, emb_ref[...], across_rows, preferred_element_type=F32)
    copies[4].wait()
    hyper = jnp.dot(chosen.astype(BF16), gen_in_ref[...], preferred_element_type=F32)
    hyper = (hyper * (1.0 / (1.0 + jnp.exp(-hyper)))).astype(BF16)
    hyper_ref[...] = hyper
    ht_ref[...] = lax.dot_general(hyper, member, across_rows, preferred_element_type=F32)
    copies[5].wait()
    for side in range(2):
        for source, target, size in blocks:
            begin = source + shift * (core if side == 0 else 1 - core)
            toks_ref[side * half + target : side * half + target + size, :] = rows_of(
                tok_ref, begin, size
            )
    x = toks_ref[:, pl.ds(pl.multiple_of(lax.axis_index("col") * slab, 128), slab)] if x_in is None else x_in[...]
    xt = x.T
    copies[6].wait()
    part = hidden // 4

    def body(i, acc):
        h = pl.multiple_of(i * part, part)
        t = jnp.dot(
            a_ref[pl.ds(pl.multiple_of(h * rank, part * rank), part * rank), :],
            xt,
            preferred_element_type=F32,
        ).reshape(part, rank, rows)
        return acc + jnp.sum(t * ht_ref[pl.ds(h, part), :][:, None, :], axis=0)

    low = lax.fori_loop(0, hidden // part, body, jnp.zeros((rank, rows), F32))
    low_ref[...] = low
    copies[7].wait()
    ff = w_ref.shape[1]
    tile = halves_of(ff)
    for j in range(0, ff, tile):
        split_store(toks_ref[...], w_ref, kept_ref, sent_ref, slice(j, j + tile))


def low_part(blocks, shift, count, task, request, tokens, emb, gen_in, a, w, x):
    hidden, slab, rank = a.shape
    groups, rows = count.shape[1], request.shape[1]
    width, ff = w.shape
    a = a.transpose(0, 2, 1).reshape(hidden * rank, slab)
    vmem = pl.BlockSpec(memory_space=pltpu.VMEM)
    hbm = pl.BlockSpec(memory_space=pltpu.HBM)
    moved = (count, task, request, tokens, emb, gen_in, a, w)
    extra = () if x is None else (x,)
    return pl.pallas_call(
        functools.partial(low_kernel, blocks, slab, shift),
        in_specs=[hbm] * len(moved) + [vmem] * len(extra),
        out_specs=[vmem] * 6,
        out_shape=(
            jax.ShapeDtypeStruct((rank, rows), F32),
            jax.ShapeDtypeStruct((groups, hidden), BF16),
            jax.ShapeDtypeStruct((groups, rows // 2), BF16),
            jax.ShapeDtypeStruct((rows, width), BF16),
            jax.ShapeDtypeStruct((rows // 2, ff), F32),
            jax.ShapeDtypeStruct((rows // 2, ff), BF16),
        ),
        scratch_shapes=[pltpu.VMEM(m.shape, m.dtype) for m in moved]
        + [pltpu.VMEM((hidden, rows), F32), pltpu.SemaphoreType.DMA((len(moved),))],
        compiler_params=pltpu.CompilerParams(vmem_limit_bytes=36 << 20),
        name="low_part",
    )(*[stay(m) for m in moved], *extra)


def split_kernel(x_ref, w_ref, kept_ref, sent_ref):
    split_store(x_ref[...], w_ref, kept_ref, sent_ref, slice(None))


def split_matmul(x, w):
    rows, width = x.shape
    ff = w.shape[1]
    tile = halves_of(ff)
    return pl.pallas_call(
        split_kernel,
        grid=(ff // tile,),
        in_specs=[
            pl.BlockSpec((rows, width), lambda i: (0, 0)),
            pl.BlockSpec((width, tile), lambda i: (0, i)),
        ],
        out_specs=[
            pl.BlockSpec((rows // 2, tile), lambda i: (0, i)),
            pl.BlockSpec((rows // 2, tile), lambda i: (0, i)),
        ],
        out_shape=(
            pltpu.VMEM((rows // 2, ff), F32),
            jax.ShapeDtypeStruct((rows // 2, ff), BF16),
        ),
        compiler_params=pltpu.CompilerParams(vmem_limit_bytes=16 << 20),
    )(x, w)


def factor_kernel(hyper_ref, gen_ref, out_ref, wide_ref):
    hidden, ranks, tile = gen_ref.shape
    groups = hyper_ref.shape[0]

    @pl.when(pl.program_id(0) == 0)
    def _():
        part = 128
        spread = part * ranks
        lane = lax.broadcasted_iota(jnp.int32, (part, spread), 1)
        first = lax.broadcasted_iota(jnp.int32, (part, spread), 0) * ranks
        repeat = ((lane >= first) & (lane < first + ranks)).astype(F32).astype(BF16)
        which = lax.rem(lax.broadcasted_iota(jnp.int32, (groups, spread), 1), ranks)
        for k in range(hidden // part):
            wide = jnp.dot(
                hyper_ref[:, k * part : (k + 1) * part], repeat, preferred_element_type=F32
            )
            for r in range(ranks):
                wide_ref[r * groups : (r + 1) * groups, k * spread : (k + 1) * spread] = jnp.where(
                    which == r, wide, 0.0
                ).astype(BF16)

    out_ref[...] = jnp.dot(
        wide_ref[...], gen_ref[...].reshape(hidden * ranks, tile), preferred_element_type=F32
    ).astype(BF16)


def factors(hyper, gen_b):
    hidden, ranks, ff = gen_b.shape
    groups = hyper.shape[0]
    tile = halves_of(ff)
    return pl.pallas_call(
        factor_kernel,
        grid=(ff // tile,),
        in_specs=[
            pl.BlockSpec((groups, hidden), lambda i: (0, 0)),
            pl.BlockSpec((hidden, ranks, tile), lambda i: (0, 0, i)),
        ],
        out_specs=pl.BlockSpec((ranks * groups, tile), lambda i: (0, i)),
        out_shape=jax.ShapeDtypeStruct((ranks * groups, ff), BF16),
        scratch_shapes=[pltpu.VMEM((ranks * groups, hidden * ranks), BF16)],
        compiler_params=pltpu.CompilerParams(vmem_limit_bytes=24 << 20),
        name="factors",
    )(hyper, gen_b)


def delta_kernel(pieces, low_ref, member_ref, mine_ref, peer_ref, kept_ref, got_ref, sum_ref, *sent):
    groups = member_ref.shape[0]
    ranks = mine_ref.shape[0] // groups
    member = member_ref[...].astype(F32)
    total = kept_ref[...] + got_ref[...].astype(F32)
    for which, factor in ((0, mine_ref), (1, peer_ref)):
        first = (lax.axis_index("row") ^ which) * ranks
        spread = jnp.concatenate(
            [
                (member * low_ref[pl.ds(first + r, 1), :].astype(BF16).astype(F32)).astype(BF16)
                for r in range(ranks)
            ],
            axis=0,
        )
        total += lax.dot_general(
            spread, factor[...], (((0,), (0,)), ((), ())), preferred_element_type=F32
        )
    sum_ref[...] = total
    total = total.astype(BF16)
    for (start, size), ref in zip(pieces, sent):
        ref[...] = total[start : start + size]


def add_adapter(pieces, low, member, mine, peer, kept, got):
    rows, ff = kept.shape
    tile = halves_of(ff)
    whole = lambda x: pl.BlockSpec(x.shape, lambda i: (0, 0))
    cut = lambda n: pl.BlockSpec((n, tile), lambda i: (0, i))
    return pl.pallas_call(
        functools.partial(delta_kernel, pieces),
        grid=(ff // tile,),
        in_specs=[whole(low), whole(member)] + [cut(x.shape[0]) for x in (mine, peer, kept, got)],
        out_specs=[cut(rows)] + [cut(size) for _, size in pieces],
        out_shape=[pltpu.VMEM((rows, ff), F32)]
        + [jax.ShapeDtypeStruct((size, ff), BF16) for _, size in pieces],
        compiler_params=pltpu.CompilerParams(vmem_limit_bytes=16 << 20),
        name="adapter",
    )(low, member, mine, peer, kept, got)


def gate_kernel(kept_ref, core_ref, rest_ref, later_ref, out_ref):
    gate = kept_ref[...] + core_ref[...].astype(F32) + rest_ref[...].astype(F32)
    out_ref[...] = gate * (1.0 / (1.0 + jnp.exp(-gate)))


def activate(kept, core_got, rest, later):
    return in_vmem(gate_kernel, pltpu.VMEM(kept.shape, F32), kept, core_got, rest, later)


def in_vmem(kernel, out, *args, scratch=()):
    vmem = pl.BlockSpec(memory_space=pltpu.VMEM)
    return pl.pallas_call(
        kernel,
        in_specs=[vmem] * len(args),
        out_specs=jax.tree.map(lambda _: vmem, out),
        out_shape=out,
        scratch_shapes=scratch,
        compiler_params=pltpu.CompilerParams(vmem_limit_bytes=8 << 20),
    )(*args)


def split_rows(hid_ref, w_ref):
    acc = jnp.dot(hid_ref[...], w_ref[...], preferred_element_type=F32)
    col = lax.axis_size("col")
    acc = acc.reshape(col // 2, 2, acc.shape[0] // col, acc.shape[1])
    low_bit = (lax.axis_index("col") & 1) == 0
    keep = jnp.where(low_bit, acc[:, 0], acc[:, 1])
    give = jnp.where(low_bit, acc[:, 1], acc[:, 0])
    return keep, give.astype(BF16)


def down_kernel(hid_ref, w_ref, keep_ref, give_ref):
    keep_ref[...], give_ref[...] = split_rows(hid_ref, w_ref)


def cross_kernel(hid_ref, w_ref, own_keep_ref, own_give_ref, keep_ref, give_ref):
    keep_ref[0], give_ref[0] = own_keep_ref[...], own_give_ref[...]
    keep_ref[1], give_ref[1] = split_rows(hid_ref, w_ref)


def down(hid, w):
    col = lax.axis_size("col")
    shape = (col // 2, hid.shape[0] // col, w.shape[1])
    out = (jax.ShapeDtypeStruct(shape, F32), jax.ShapeDtypeStruct(shape, BF16))
    return in_vmem(down_kernel, out, hid, w)


def cross(other, w, own):
    out = tuple(jax.ShapeDtypeStruct((2,) + x.shape, x.dtype) for x in own)
    return in_vmem(cross_kernel, out, other, w, *own)


def turned_split(hid_ref, w_ref, scratch):
    acc = jnp.dot(hid_ref[...], w_ref[...], preferred_element_type=F32)
    col = lax.axis_size("col")
    scratch[...] = acc.reshape(col // 2, 2, acc.shape[0] // col, acc.shape[1])
    here = lax.axis_index("col") >> 1
    return [scratch[pl.ds(here ^ q, 1)][0] for q in range(4)]


def turned_down_kernel(hid_ref, w_ref, *refs):
    for part, ref in zip(turned_split(hid_ref, w_ref, refs[4]), refs):
        ref[...] = part.astype(ref.dtype)


def turned_cross_kernel(hid_ref, w_ref, *refs):
    for part, own, ref in zip(turned_split(hid_ref, w_ref, refs[8]), refs[:4], refs[4:]):
        ref[0] = own[...]
        ref[1] = part.astype(ref.dtype)


def turned_down(hid, w, own):
    col = lax.axis_size("col")
    shape = (2, hid.shape[0] // col, w.shape[1])
    scratch = [pltpu.VMEM((col // 2,) + shape, F32)]
    lead = () if own is None else (2,)
    out = [jax.ShapeDtypeStruct(lead + shape, F32 if q == 0 else BF16) for q in range(4)]
    kernel, own = (turned_down_kernel, ()) if own is None else (turned_cross_kernel, own)
    return in_vmem(kernel, out, hid, w, *own, scratch=scratch)


def turned_fold_kernel(total_ref, *refs):
    side = lax.axis_index("col") & 1
    for ref, which in ((refs[3], side), (refs[4], 1 - side)):
        at = pl.ds(which, 1)
        value = total_ref[:, at]
        for got in refs[:3]:
            value += got[:, at].astype(F32)
        ref[...] = value.astype(ref.dtype)


def turned_fold(total, gots):
    shape = total.shape[:1] + (1,) + total.shape[2:]
    out = (jax.ShapeDtypeStruct(shape, F32), jax.ShapeDtypeStruct(shape, BF16))
    return in_vmem(turned_fold_kernel, out, total, *gots)


def fold_kernel(bit, keep_ref, got_ref, new_ref, give_ref):
    parts = keep_ref.shape[1]
    side = (lax.axis_index("col") >> bit) & 1
    for j in range(parts // 2):
        for ref, which in ((new_ref, side), (give_ref, 1 - side)):
            at = pl.ds(2 * j + which, 1)
            ref[:, j : j + 1] = (keep_ref[:, at] + got_ref[:, at].astype(F32)).astype(ref.dtype)


def fold(bit, keep, got):
    shape = keep.shape[:1] + (keep.shape[1] // 2,) + keep.shape[2:]
    out = (jax.ShapeDtypeStruct(shape, F32), jax.ShapeDtypeStruct(shape, BF16))
    return in_vmem(functools.partial(fold_kernel, bit), out, keep, got)


def last_kernel(bit, count, *refs):
    here = lax.axis_index("col") >> bit
    start = 0
    for k in range(count):
        keep_ref, got_ref = refs[2 * k : 2 * k + 2]
        rows = slice(start, start + keep_ref.shape[2])
        for q, ref in enumerate(refs[2 * count :]):
            at = pl.ds(here ^ q, 1)
            ref[:, :, rows] = (keep_ref[:, at] + got_ref[:, at].astype(F32)).astype(ref.dtype)
        start = rows.stop


def last_split(bit, parts):
    keep = parts[0][0]
    shape = keep.shape[:1] + (1, sum(k.shape[2] for k, _ in parts)) + keep.shape[3:]
    out = [jax.ShapeDtypeStruct(shape, F32)] + [jax.ShapeDtypeStruct(shape, BF16)] * 3
    kernel = functools.partial(last_kernel, bit, len(parts))
    return in_vmem(kernel, out, *[x for part in parts for x in part])


def join_kernel(counts, *refs):
    out_ref = refs[-1]
    requests, draft, width = out_ref.shape
    core = lax.axis_index("row") & 1
    start = 0
    for count in counts:
        (total, *got), refs = refs[:count], refs[count:]
        for side in range(2):
            value = total[side, 0]
            for g in got:
                value += g[side, 0].astype(F32)
            size = value.shape[0] // draft
            at = start + (requests // 2) * (core if side == 0 else 1 - core)
            out_ref[pl.ds(at, size)] = value.astype(BF16).reshape(size, draft, width)
        start += size


def join(parts, out):
    kernel = functools.partial(join_kernel, tuple(len(p) for p in parts))
    return in_vmem(kernel, out, *[x for p in parts for x in p])


def hidden_kernel(start, act_ref, half_ref, up_ref, out_ref):
    at = slice(start, start + out_ref.shape[0])
    out_ref[...] = (act_ref[at] * (half_ref[at] + up_ref[...].astype(F32))).astype(BF16)


def hidden_units(piece, act, half, up_got):
    start, size = piece
    out = jax.ShapeDtypeStruct((size, act.shape[1]), BF16)
    return in_vmem(functools.partial(hidden_kernel, start), out, act, half, up_got)


def shards(tokens, task_emb, gen_in, gen_a, gen_b, w_gate, w_up, w_down, group_count, group_task):
    batch, draft, _ = tokens.shape
    rows = batch * draft
    rn, cn = lax.axis_size("row"), lax.axis_size("col")
    ri, ci = lax.axis_index("row"), lax.axis_index("col")
    core = ri & 1
    rmasks, cmasks = masks_of(rn), masks_of(cn)
    slab = gen_a.shape[1]

    per_dest = rows // cn
    chunks, joint, turned = plan(per_dest)
    turned = turned and len(cmasks) == 3
    sizes = [per_dest * part // sum(chunks) for part in chunks]
    blocks, pieces, target, source = [], [], 0, 0
    for size in sizes:
        pieces.append((target, cn * size // 2))
        for d in range(cn):
            blocks.append(((d * per_dest + source) // draft, target, size // 2))
            target += size // 2
        source += size // 2
    shift = per_dest // 2 // draft

    request = np.concatenate([begin + np.arange(size) // draft for begin, _, size in blocks])
    request = np.concatenate([request, request])[None, :].astype(np.int32)
    x = None
    if slab % 128:
        x = lax.dynamic_slice_in_dim(tokens, ci * slab, slab, 2)
        x = jnp.concatenate(
            [
                lax.dynamic_slice_in_dim(x, begin + shift * side, size // draft).reshape(size, slab)
                for side in (core, 1 - core)
                for begin, _, size in blocks
            ]
        )
    low, hyper, own_member, toks, gate_kept, gate_sent = low_part(
        tuple(blocks),
        shift,
        group_count[None, :],
        group_task[None, :],
        jnp.asarray(request),
        tokens,
        task_emb,
        gen_in,
        gen_a,
        w_gate,
        x,
    )
    gate_got = swap(gate_sent, "row", 1)
    for m in rmasks[1:]:
        low = low + swap(low, "row", m)
    gate_sum = (gate_kept + gate_got.astype(F32)).astype(BF16)

    def others(sent):
        total = None
        for s, m in enumerate(rmasks[1:]):
            got = swap(sent, "row", m)
            if s + 2 == len(rmasks) and total is None:
                return got
            total = got.astype(F32) if total is None else total + got.astype(F32)
            sent = (sent.astype(F32) + got.astype(F32)).astype(BF16)
        return total

    gate_rest = others(gate_sum)

    up_kept, up_sent = split_matmul(toks, w_up)
    up_got = swap(up_sent, "row", 1)
    b_mine = factors(hyper, gen_b)
    b_peer = swap(b_mine, "row", 1)
    for m in cmasks[:-2]:
        low = low + swap(low, "col", m)
    gots = [swap(low, "col", q * cmasks[-2]) for q in (1, 2, 3)]
    low = low + gots[0] + gots[1] + gots[2]
    low = low[:, : rows // 2] + swap(low[:, rows // 2 :], "row", 1)

    up_half, *up_sums = add_adapter(
        tuple(pieces), low, own_member, b_mine, b_peer, up_kept, up_got
    )

    act = activate(gate_kept, gate_got, gate_rest, w_down)
    outs = []
    for k, piece in enumerate(pieces):
        up_rest = others(up_sums[k])
        hid = hidden_units(piece, act, up_half, up_rest)
        other = swap(hid, "row", 1)
        if k == 0 and turned:
            own = turned_down(hid, w_down, None)
            total, *gives = turned_down(other, w_down, own)
            gots = [swap(give, "col", (q + 1) << 1) for q, give in enumerate(gives)]
            keep, give = turned_fold(total, gots)
            first = [keep, swap(give, "col", 1)]
            outs.append(None)
            continue
        keep, give = cross(other, w_down, down(hid, w_down))
        for s, m in enumerate(cmasks[:-2]):
            got = swap(give, "col", m)
            if s + 3 < len(cmasks):
                keep, give = fold(s + 1, keep, got)
        outs.append((keep, got))
    low_bit = len(cmasks) - 2
    parts = [first] if turned else []
    for members in joint:
        total, *gives = last_split(low_bit, [outs[k] for k in members])
        gots = [swap(give, "col", (q + 1) << low_bit) for q, give in enumerate(gives)]
        parts.append([total] + gots)
    return join(parts, jax.ShapeDtypeStruct((batch // cn, draft, w_down.shape[1]), BF16))


def solution(mesh):
    in_specs = (
        P(None, None, "row"),
        P(),
        P(),
        P(None, ("row", "col"), None),
        P(None, "row", "col"),
        P("row", "col"),
        P("row", "col"),
        P("col", "row"),
        P(),
        P(),
    )
    out_specs = P("col", None, "row")

    return jax.shard_map(shards, mesh=mesh, in_specs=in_specs, out_specs=out_specs, check_vma=False)
```

```python
import functools

import jax
import jax.numpy as jnp
import numpy as np
from jax import lax
from jax.experimental import pallas as pl
from jax.experimental.pallas import tpu as pltpu
from jax.sharding import PartitionSpec as P


F32 = jnp.float32
BF16 = jnp.bfloat16
ROW, COL = "row", "col"


def plan(per_dest):
    if per_dest % 64 == 0:
        return (1, 1, 1, 1), ((1, 2), (3,)), True
    return (1, 1), ((0,), (1,)), False


def swap(x, axis, mask):
    n = lax.axis_size(axis)
    return lax.ppermute(x, axis, [(i, i ^ mask) for i in range(n)])


def masks_of(n):
    return [1 << b for b in range(n.bit_length() - 1)]


def stay(x):
    return pltpu.with_memory_space_constraint(x, pltpu.HBM)


def halves_of(n):
    return n // 2 if (n // 2) % 128 == 0 else n


def rows_of(tok_ref, request, size):
    draft, width = tok_ref.shape[1:]
    return tok_ref[pl.ds(request, size // draft)].reshape(size, width)


def split_store(x, w_ref, kept_ref, sent_ref, columns):
    half = x.shape[0] // 2
    both = jnp.dot(x, w_ref[:, columns], preferred_element_type=F32)
    kept_ref[:, columns] = both[:half]
    sent_ref[:, columns] = both[half:].astype(BF16)


def low_kernel(
    blocks, slab, shift, count_hbm, task_hbm, request_hbm, tok_hbm, emb_hbm, gen_in_hbm, a_hbm,
    w_hbm, *rest
):
    x_in, rest = (None, rest) if slab % 128 == 0 else (rest[0], rest[1:])
    low_ref, hyper_ref, member_ref, toks_ref, kept_ref, sent_ref = rest[:6]
    count_ref, task_ref, request_ref, tok_ref, emb_ref, gen_in_ref, a_ref, w_ref, ht_ref, sems = rest[6:]
    copies = [
        pltpu.make_async_copy(src, dst, sems.at[i])
        for i, (src, dst) in enumerate(
            (
                (task_hbm, task_ref),
                (count_hbm, count_ref),
                (request_hbm, request_ref),
                (emb_hbm, emb_ref),
                (gen_in_hbm, gen_in_ref),
                (tok_hbm, tok_ref),
                (a_hbm, a_ref),
                (w_hbm, w_ref),
            )
        )
    ]
    for copy in copies:
        copy.start()
    groups = count_ref.shape[1]
    tasks = emb_ref.shape[0]
    hidden = gen_in_ref.shape[1]
    rank, rows = low_ref.shape
    half = rows // 2
    core = lax.axis_index(ROW) & 1
    across_rows = (((0,), (0,)), ((), ()))
    for copy in copies[:3]:
        copy.wait()
    chosen = lax.broadcasted_iota(jnp.int32, (tasks, groups), 0) == task_ref[...]
    chosen = chosen.astype(F32).astype(BF16)
    at = lax.broadcasted_iota(jnp.int32, (groups, groups), 0)
    of = lax.broadcasted_iota(jnp.int32, (groups, groups), 1)
    ends = jnp.sum(jnp.where(of <= at, count_ref[...], 0), axis=1, keepdims=True)
    starts = jnp.sum(jnp.where(of < at, count_ref[...], 0), axis=1, keepdims=True)
    first = lax.broadcasted_iota(jnp.int32, (1, rows), 1) < half
    request = request_ref[...] + shift * jnp.where(first, core, 1 - core)
    member = ((request >= starts) & (request < ends)).astype(F32).astype(BF16)
    member_ref[...] = member[:, :half]
    copies[3].wait()
    chosen = lax.dot_general(chosen, emb_ref[...], across_rows, preferred_element_type=F32)
    copies[4].wait()
    hyper = jnp.dot(chosen.astype(BF16), gen_in_ref[...], preferred_element_type=F32)
    hyper = (hyper * (1.0 / (1.0 + jnp.exp(-hyper)))).astype(BF16)
    hyper_ref[...] = hyper
    ht_ref[...] = lax.dot_general(hyper, member, across_rows, preferred_element_type=F32)
    copies[5].wait()
    for side in range(2):
        for source, target, size in blocks:
            begin = source + shift * (core if side == 0 else 1 - core)
            toks_ref[side * half + target : side * half + target + size, :] = rows_of(
                tok_ref, begin, size
            )
    x = toks_ref[:, pl.ds(pl.multiple_of(lax.axis_index(COL) * slab, 128), slab)] if x_in is None else x_in[...]
    xt = x.T
    copies[6].wait()
    part = hidden // 4

    def body(i, acc):
        h = pl.multiple_of(i * part, part)
        t = jnp.dot(
            a_ref[pl.ds(pl.multiple_of(h * rank, part * rank), part * rank), :],
            xt,
            preferred_element_type=F32,
        ).reshape(part, rank, rows)
        return acc + jnp.sum(t * ht_ref[pl.ds(h, part), :][:, None, :], axis=0)

    low = lax.fori_loop(0, hidden // part, body, jnp.zeros((rank, rows), F32))
    low_ref[...] = low
    copies[7].wait()
    ff = w_ref.shape[1]
    tile = halves_of(ff)
    for j in range(0, ff, tile):
        split_store(toks_ref[...], w_ref, kept_ref, sent_ref, slice(j, j + tile))


def low_part(blocks, shift, count, task, request, tokens, emb, gen_in, a, w, x):
    hidden, slab, rank = a.shape
    groups, rows = count.shape[1], request.shape[1]
    width, ff = w.shape
    a = a.transpose(0, 2, 1).reshape(hidden * rank, slab)
    vmem = pl.BlockSpec(memory_space=pltpu.VMEM)
    hbm = pl.BlockSpec(memory_space=pltpu.HBM)
    moved = (count, task, request, tokens, emb, gen_in, a, w)
    extra = () if x is None else (x,)
    return pl.pallas_call(
        functools.partial(low_kernel, blocks, slab, shift),
        in_specs=[hbm] * len(moved) + [vmem] * len(extra),
        out_specs=[vmem] * 6,
        out_shape=(
            jax.ShapeDtypeStruct((rank, rows), F32),
            jax.ShapeDtypeStruct((groups, hidden), BF16),
            jax.ShapeDtypeStruct((groups, rows // 2), BF16),
            jax.ShapeDtypeStruct((rows, width), BF16),
            jax.ShapeDtypeStruct((rows // 2, ff), F32),
            jax.ShapeDtypeStruct((rows // 2, ff), BF16),
        ),
        scratch_shapes=[pltpu.VMEM(m.shape, m.dtype) for m in moved]
        + [pltpu.VMEM((hidden, rows), F32), pltpu.SemaphoreType.DMA((len(moved),))],
        compiler_params=pltpu.CompilerParams(vmem_limit_bytes=36 << 20),
        name="low_part",
    )(*[stay(m) for m in moved], *extra)


def split_kernel(x_ref, w_ref, kept_ref, sent_ref):
    split_store(x_ref[...], w_ref, kept_ref, sent_ref, slice(None))


def split_matmul(x, w):
    rows, width = x.shape
    ff = w.shape[1]
    tile = halves_of(ff)
    return pl.pallas_call(
        split_kernel,
        grid=(ff // tile,),
        in_specs=[
            pl.BlockSpec((rows, width), lambda i: (0, 0)),
            pl.BlockSpec((width, tile), lambda i: (0, i)),
        ],
        out_specs=[
            pl.BlockSpec((rows // 2, tile), lambda i: (0, i)),
            pl.BlockSpec((rows // 2, tile), lambda i: (0, i)),
        ],
        out_shape=(
            pltpu.VMEM((rows // 2, ff), F32),
            jax.ShapeDtypeStruct((rows // 2, ff), BF16),
        ),
        compiler_params=pltpu.CompilerParams(vmem_limit_bytes=16 << 20),
    )(x, w)


def factor_kernel(hyper_ref, gen_ref, out_ref, wide_ref):
    hidden, ranks, tile = gen_ref.shape
    groups = hyper_ref.shape[0]

    @pl.when(pl.program_id(0) == 0)
    def _():
        part = 128
        spread = part * ranks
        lane = lax.broadcasted_iota(jnp.int32, (part, spread), 1)
        first = lax.broadcasted_iota(jnp.int32, (part, spread), 0) * ranks
        repeat = ((lane >= first) & (lane < first + ranks)).astype(F32).astype(BF16)
        which = lax.rem(lax.broadcasted_iota(jnp.int32, (groups, spread), 1), ranks)
        for k in range(hidden // part):
            wide = jnp.dot(
                hyper_ref[:, k * part : (k + 1) * part], repeat, preferred_element_type=F32
            )
            for r in range(ranks):
                wide_ref[r * groups : (r + 1) * groups, k * spread : (k + 1) * spread] = jnp.where(
                    which == r, wide, 0.0
                ).astype(BF16)

    out_ref[...] = jnp.dot(
        wide_ref[...], gen_ref[...].reshape(hidden * ranks, tile), preferred_element_type=F32
    ).astype(BF16)


def factors(hyper, gen_b):
    hidden, ranks, ff = gen_b.shape
    groups = hyper.shape[0]
    tile = halves_of(ff)
    return pl.pallas_call(
        factor_kernel,
        grid=(ff // tile,),
        in_specs=[
            pl.BlockSpec((groups, hidden), lambda i: (0, 0)),
            pl.BlockSpec((hidden, ranks, tile), lambda i: (0, 0, i)),
        ],
        out_specs=pl.BlockSpec((ranks * groups, tile), lambda i: (0, i)),
        out_shape=jax.ShapeDtypeStruct((ranks * groups, ff), BF16),
        scratch_shapes=[pltpu.VMEM((ranks * groups, hidden * ranks), BF16)],
        compiler_params=pltpu.CompilerParams(vmem_limit_bytes=24 << 20),
        name="factors",
    )(hyper, gen_b)


def delta_kernel(pieces, low_ref, member_ref, mine_ref, peer_ref, kept_ref, got_ref, sum_ref, *sent):
    groups = member_ref.shape[0]
    ranks = mine_ref.shape[0] // groups
    member = member_ref[...].astype(F32)
    total = kept_ref[...] + got_ref[...].astype(F32)
    for which, factor in ((0, mine_ref), (1, peer_ref)):
        first = (lax.axis_index(ROW) ^ which) * ranks
        spread = jnp.concatenate(
            [
                (member * low_ref[pl.ds(first + r, 1), :].astype(BF16).astype(F32)).astype(BF16)
                for r in range(ranks)
            ],
            axis=0,
        )
        total += lax.dot_general(
            spread, factor[...], (((0,), (0,)), ((), ())), preferred_element_type=F32
        )
    sum_ref[...] = total
    total = total.astype(BF16)
    for (start, size), ref in zip(pieces, sent):
        ref[...] = total[start : start + size]


def add_adapter(pieces, low, member, mine, peer, kept, got):
    rows, ff = kept.shape
    tile = halves_of(ff)
    whole = lambda x: pl.BlockSpec(x.shape, lambda i: (0, 0))
    cut = lambda n: pl.BlockSpec((n, tile), lambda i: (0, i))
    return pl.pallas_call(
        functools.partial(delta_kernel, pieces),
        grid=(ff // tile,),
        in_specs=[whole(low), whole(member)] + [cut(x.shape[0]) for x in (mine, peer, kept, got)],
        out_specs=[cut(rows)] + [cut(size) for _, size in pieces],
        out_shape=[pltpu.VMEM((rows, ff), F32)]
        + [jax.ShapeDtypeStruct((size, ff), BF16) for _, size in pieces],
        compiler_params=pltpu.CompilerParams(vmem_limit_bytes=16 << 20),
        name="adapter",
    )(low, member, mine, peer, kept, got)


def gate_kernel(kept_ref, core_ref, rest_ref, later_ref, out_ref):
    gate = kept_ref[...] + core_ref[...].astype(F32) + rest_ref[...].astype(F32)
    out_ref[...] = gate * (1.0 / (1.0 + jnp.exp(-gate)))


def activate(kept, core_got, rest, later):
    return in_vmem(gate_kernel, pltpu.VMEM(kept.shape, F32), kept, core_got, rest, later)


def in_vmem(kernel, out, *args, scratch=()):
    vmem = pl.BlockSpec(memory_space=pltpu.VMEM)
    return pl.pallas_call(
        kernel,
        in_specs=[vmem] * len(args),
        out_specs=jax.tree.map(lambda _: vmem, out),
        out_shape=out,
        scratch_shapes=scratch,
        compiler_params=pltpu.CompilerParams(vmem_limit_bytes=8 << 20),
    )(*args)


def split_rows(hid_ref, w_ref):
    acc = jnp.dot(hid_ref[...], w_ref[...], preferred_element_type=F32)
    col = lax.axis_size(COL)
    acc = acc.reshape(col // 2, 2, acc.shape[0] // col, acc.shape[1])
    low_bit = (lax.axis_index(COL) & 1) == 0
    keep = jnp.where(low_bit, acc[:, 0], acc[:, 1])
    give = jnp.where(low_bit, acc[:, 1], acc[:, 0])
    return keep, give.astype(BF16)


def down_kernel(hid_ref, w_ref, keep_ref, give_ref):
    keep_ref[...], give_ref[...] = split_rows(hid_ref, w_ref)


def cross_kernel(hid_ref, w_ref, own_keep_ref, own_give_ref, keep_ref, give_ref):
    keep_ref[0], give_ref[0] = own_keep_ref[...], own_give_ref[...]
    keep_ref[1], give_ref[1] = split_rows(hid_ref, w_ref)


def down(hid, w):
    col = lax.axis_size(COL)
    shape = (col // 2, hid.shape[0] // col, w.shape[1])
    out = (jax.ShapeDtypeStruct(shape, F32), jax.ShapeDtypeStruct(shape, BF16))
    return in_vmem(down_kernel, out, hid, w)


def cross(other, w, own):
    out = tuple(jax.ShapeDtypeStruct((2,) + x.shape, x.dtype) for x in own)
    return in_vmem(cross_kernel, out, other, w, *own)


def turned_split(hid_ref, w_ref, scratch):
    acc = jnp.dot(hid_ref[...], w_ref[...], preferred_element_type=F32)
    col = lax.axis_size(COL)
    scratch[...] = acc.reshape(col // 2, 2, acc.shape[0] // col, acc.shape[1])
    here = lax.axis_index(COL) >> 1
    return [scratch[pl.ds(here ^ q, 1)][0] for q in range(4)]


def turned_down_kernel(hid_ref, w_ref, *refs):
    for part, ref in zip(turned_split(hid_ref, w_ref, refs[4]), refs):
        ref[...] = part.astype(ref.dtype)


def turned_cross_kernel(hid_ref, w_ref, *refs):
    for part, own, ref in zip(turned_split(hid_ref, w_ref, refs[8]), refs[:4], refs[4:]):
        ref[0] = own[...]
        ref[1] = part.astype(ref.dtype)


def turned_down(hid, w, own):
    col = lax.axis_size(COL)
    shape = (2, hid.shape[0] // col, w.shape[1])
    scratch = [pltpu.VMEM((col // 2,) + shape, F32)]
    lead = () if own is None else (2,)
    out = [jax.ShapeDtypeStruct(lead + shape, F32 if q == 0 else BF16) for q in range(4)]
    kernel, own = (turned_down_kernel, ()) if own is None else (turned_cross_kernel, own)
    return in_vmem(kernel, out, hid, w, *own, scratch=scratch)


def turned_fold_kernel(total_ref, *refs):
    side = lax.axis_index(COL) & 1
    for ref, which in ((refs[3], side), (refs[4], 1 - side)):
        at = pl.ds(which, 1)
        value = total_ref[:, at]
        for got in refs[:3]:
            value += got[:, at].astype(F32)
        ref[...] = value.astype(ref.dtype)


def turned_fold(total, gots):
    shape = total.shape[:1] + (1,) + total.shape[2:]
    out = (jax.ShapeDtypeStruct(shape, F32), jax.ShapeDtypeStruct(shape, BF16))
    return in_vmem(turned_fold_kernel, out, total, *gots)


def fold_kernel(bit, keep_ref, got_ref, new_ref, give_ref):
    parts = keep_ref.shape[1]
    side = (lax.axis_index(COL) >> bit) & 1
    for j in range(parts // 2):
        for ref, which in ((new_ref, side), (give_ref, 1 - side)):
            at = pl.ds(2 * j + which, 1)
            ref[:, j : j + 1] = (keep_ref[:, at] + got_ref[:, at].astype(F32)).astype(ref.dtype)


def fold(bit, keep, got):
    shape = keep.shape[:1] + (keep.shape[1] // 2,) + keep.shape[2:]
    out = (jax.ShapeDtypeStruct(shape, F32), jax.ShapeDtypeStruct(shape, BF16))
    return in_vmem(functools.partial(fold_kernel, bit), out, keep, got)


def last_kernel(bit, count, *refs):
    here = lax.axis_index(COL) >> bit
    start = 0
    for k in range(count):
        keep_ref, got_ref = refs[2 * k : 2 * k + 2]
        rows = slice(start, start + keep_ref.shape[2])
        for q, ref in enumerate(refs[2 * count :]):
            at = pl.ds(here ^ q, 1)
            ref[:, :, rows] = (keep_ref[:, at] + got_ref[:, at].astype(F32)).astype(ref.dtype)
        start = rows.stop


def last_split(bit, parts):
    keep = parts[0][0]
    shape = keep.shape[:1] + (1, sum(k.shape[2] for k, _ in parts)) + keep.shape[3:]
    out = [jax.ShapeDtypeStruct(shape, F32)] + [jax.ShapeDtypeStruct(shape, BF16)] * 3
    kernel = functools.partial(last_kernel, bit, len(parts))
    return in_vmem(kernel, out, *[x for part in parts for x in part])


def join_kernel(counts, *refs):
    out_ref = refs[-1]
    requests, draft, width = out_ref.shape
    core = lax.axis_index(ROW) & 1
    start = 0
    for count in counts:
        (total, *got), refs = refs[:count], refs[count:]
        for side in range(2):
            value = total[side, 0]
            for g in got:
                value += g[side, 0].astype(F32)
            size = value.shape[0] // draft
            at = start + (requests // 2) * (core if side == 0 else 1 - core)
            out_ref[pl.ds(at, size)] = value.astype(BF16).reshape(size, draft, width)
        start += size


def join(parts, out):
    kernel = functools.partial(join_kernel, tuple(len(p) for p in parts))
    return in_vmem(kernel, out, *[x for p in parts for x in p])


def hidden_kernel(start, act_ref, half_ref, up_ref, out_ref):
    at = slice(start, start + out_ref.shape[0])
    out_ref[...] = (act_ref[at] * (half_ref[at] + up_ref[...].astype(F32))).astype(BF16)


def hidden_units(piece, act, half, up_got):
    start, size = piece
    out = jax.ShapeDtypeStruct((size, act.shape[1]), BF16)
    return in_vmem(functools.partial(hidden_kernel, start), out, act, half, up_got)


def shards(tokens, task_emb, gen_in, gen_a, gen_b, w_gate, w_up, w_down, group_count, group_task):
    batch, draft, _ = tokens.shape
    rows = batch * draft
    rn, cn = lax.axis_size(ROW), lax.axis_size(COL)
    ri, ci = lax.axis_index(ROW), lax.axis_index(COL)
    core = ri & 1
    rmasks, cmasks = masks_of(rn), masks_of(cn)
    slab = gen_a.shape[1]

    per_dest = rows // cn
    chunks, joint, turned = plan(per_dest)
    turned = turned and len(cmasks) == 3
    sizes = [per_dest * part // sum(chunks) for part in chunks]
    blocks, pieces, target, source = [], [], 0, 0
    for size in sizes:
        pieces.append((target, cn * size // 2))
        for d in range(cn):
            blocks.append(((d * per_dest + source) // draft, target, size // 2))
            target += size // 2
        source += size // 2
    shift = per_dest // 2 // draft

    request = np.concatenate([begin + np.arange(size) // draft for begin, _, size in blocks])
    request = np.concatenate([request, request])[None, :].astype(np.int32)
    x = None
    if slab % 128:
        x = lax.dynamic_slice_in_dim(tokens, ci * slab, slab, 2)
        x = jnp.concatenate(
            [
                lax.dynamic_slice_in_dim(x, begin + shift * side, size // draft).reshape(size, slab)
                for side in (core, 1 - core)
                for begin, _, size in blocks
            ]
        )
    low, hyper, own_member, toks, gate_kept, gate_sent = low_part(
        tuple(blocks),
        shift,
        group_count[None, :],
        group_task[None, :],
        jnp.asarray(request),
        tokens,
        task_emb,
        gen_in,
        gen_a,
        w_gate,
        x,
    )
    gate_got = swap(gate_sent, ROW, 1)
    for m in rmasks[1:]:
        low = low + swap(low, ROW, m)
    gate_sum = (gate_kept + gate_got.astype(F32)).astype(BF16)

    def others(sent):
        total = None
        for s, m in enumerate(rmasks[1:]):
            got = swap(sent, ROW, m)
            if s + 2 == len(rmasks) and total is None:
                return got
            total = got.astype(F32) if total is None else total + got.astype(F32)
            sent = (sent.astype(F32) + got.astype(F32)).astype(BF16)
        return total

    gate_rest = others(gate_sum)

    up_kept, up_sent = split_matmul(toks, w_up)
    up_got = swap(up_sent, ROW, 1)
    b_mine = factors(hyper, gen_b)
    b_peer = swap(b_mine, ROW, 1)
    for m in cmasks[:-2]:
        low = low + swap(low, COL, m)
    gots = [swap(low, COL, q * cmasks[-2]) for q in (1, 2, 3)]
    low = low + gots[0] + gots[1] + gots[2]
    low = low[:, : rows // 2] + swap(low[:, rows // 2 :], ROW, 1)

    up_half, *up_sums = add_adapter(
        tuple(pieces), low, own_member, b_mine, b_peer, up_kept, up_got
    )

    act = activate(gate_kept, gate_got, gate_rest, w_down)
    outs = []
    for k, piece in enumerate(pieces):
        up_rest = others(up_sums[k])
        hid = hidden_units(piece, act, up_half, up_rest)
        other = swap(hid, ROW, 1)
        if k == 0 and turned:
            own = turned_down(hid, w_down, None)
            total, *gives = turned_down(other, w_down, own)
            gots = [swap(give, COL, (q + 1) << 1) for q, give in enumerate(gives)]
            keep, give = turned_fold(total, gots)
            first = [keep, swap(give, COL, 1)]
            outs.append(None)
            continue
        keep, give = cross(other, w_down, down(hid, w_down))
        for s, m in enumerate(cmasks[:-2]):
            got = swap(give, COL, m)
            if s + 3 < len(cmasks):
                keep, give = fold(s + 1, keep, got)
        outs.append((keep, got))
    low_bit = len(cmasks) - 2
    parts = [first] if turned else []
    for members in joint:
        total, *gives = last_split(low_bit, [outs[k] for k in members])
        gots = [swap(give, COL, (q + 1) << low_bit) for q, give in enumerate(gives)]
        parts.append([total] + gots)
    return join(parts, jax.ShapeDtypeStruct((batch // cn, draft, w_down.shape[1]), BF16))


def solution(mesh):
    in_specs = (
        P(None, None, ROW),
        P(),
        P(),
        P(None, (ROW, COL), None),
        P(None, ROW, COL),
        P(ROW, COL),
        P(ROW, COL),
        P(COL, ROW),
        P(),
        P(),
    )
    out_specs = P(COL, None, ROW)

    return jax.shard_map(shards, mesh=mesh, in_specs=in_specs, out_specs=out_specs, check_vma=False)
```

```python
import functools

import jax
import jax.numpy as jnp
import numpy as np
from jax import lax
from jax.experimental import pallas as pl
from jax.experimental.pallas import tpu as pltpu
from jax.sharding import PartitionSpec as P


F32 = jnp.float32
BF16 = jnp.bfloat16
ROW, COL = "row", "col"


def plan(per_dest):
    if per_dest % 64 == 0:
        return (1, 1, 1, 1), ((1, 2), (3,)), True
    return (1, 1), ((0,), (1,)), False


def swap(x, axis, mask):
    n = lax.axis_size(axis)
    return lax.ppermute(x, axis, [(i, i ^ mask) for i in range(n)])


def masks_of(n):
    return [1 << b for b in range(n.bit_length() - 1)]


def stay(x):
    return pltpu.with_memory_space_constraint(x, pltpu.HBM)


def halves_of(n):
    return n // 2 if (n // 2) % 128 == 0 else n


def rows_of(tok_ref, request, size):
    draft, width = tok_ref.shape[1:]
    return tok_ref[pl.ds(request, size // draft)].reshape(size, width)


def split_store(x, w_ref, kept_ref, sent_ref, columns):
    half = x.shape[0] // 2
    both = jnp.dot(x, w_ref[:, columns], preferred_element_type=F32)
    kept_ref[:, columns] = both[:half]
    sent_ref[:, columns] = both[half:].astype(BF16)


def low_kernel(
    blocks, slab, shift, count_hbm, task_hbm, request_hbm, tok_hbm, emb_hbm, gen_in_hbm, a_hbm,
    w_hbm, *rest
):
    x_in, rest = (None, rest) if slab % 128 == 0 else (rest[0], rest[1:])
    low_ref, hyper_ref, member_ref, toks_ref, kept_ref, sent_ref = rest[:6]
    count_ref, task_ref, request_ref, tok_ref, emb_ref, gen_in_ref, a_ref, w_ref, ht_ref, sems = rest[6:]
    copies = [
        pltpu.make_async_copy(src, dst, sems.at[i])
        for i, (src, dst) in enumerate(
            (
                (task_hbm, task_ref),
                (count_hbm, count_ref),
                (request_hbm, request_ref),
                (emb_hbm, emb_ref),
                (gen_in_hbm, gen_in_ref),
                (tok_hbm, tok_ref),
                (a_hbm, a_ref),
                (w_hbm, w_ref),
            )
        )
    ]
    for copy in copies:
        copy.start()
    groups = count_ref.shape[1]
    tasks = emb_ref.shape[0]
    hidden = gen_in_ref.shape[1]
    rank, rows = low_ref.shape
    half = rows // 2
    core = lax.axis_index(ROW) & 1
    across_rows = (((0,), (0,)), ((), ()))
    for copy in copies[:3]:
        copy.wait()
    chosen = lax.broadcasted_iota(jnp.int32, (tasks, groups), 0) == task_ref[...]
    chosen = chosen.astype(F32).astype(BF16)
    at = lax.broadcasted_iota(jnp.int32, (groups, groups), 0)
    of = lax.broadcasted_iota(jnp.int32, (groups, groups), 1)
    ends = jnp.sum(jnp.where(of <= at, count_ref[...], 0), axis=1, keepdims=True)
    starts = jnp.sum(jnp.where(of < at, count_ref[...], 0), axis=1, keepdims=True)
    first = lax.broadcasted_iota(jnp.int32, (1, rows), 1) < half
    request = request_ref[...] + shift * jnp.where(first, core, 1 - core)
    member = ((request >= starts) & (request < ends)).astype(F32).astype(BF16)
    member_ref[...] = member[:, :half]
    copies[3].wait()
    chosen = lax.dot_general(chosen, emb_ref[...], across_rows, preferred_element_type=F32)
    copies[4].wait()
    hyper = jnp.dot(chosen.astype(BF16), gen_in_ref[...], preferred_element_type=F32)
    hyper = (hyper * (1.0 / (1.0 + jnp.exp(-hyper)))).astype(BF16)
    hyper_ref[...] = hyper
    ht_ref[...] = lax.dot_general(hyper, member, across_rows, preferred_element_type=F32)
    copies[5].wait()
    for side in range(2):
        for source, target, size in blocks:
            begin = source + shift * (core if side == 0 else 1 - core)
            toks_ref[side * half + target : side * half + target + size, :] = rows_of(
                tok_ref, begin, size
            )
    x = toks_ref[:, pl.ds(pl.multiple_of(lax.axis_index(COL) * slab, 128), slab)] if x_in is None else x_in[...]
    xt = x.T
    copies[6].wait()
    part = hidden // 4

    def body(i, acc):
        h = pl.multiple_of(i * part, part)
        t = jnp.dot(
            a_ref[pl.ds(pl.multiple_of(h * rank, part * rank), part * rank), :],
            xt,
            preferred_element_type=F32,
        ).reshape(part, rank, rows)
        return acc + jnp.sum(t * ht_ref[pl.ds(h, part), :][:, None, :], axis=0)

    low = lax.fori_loop(0, hidden // part, body, jnp.zeros((rank, rows), F32))
    low_ref[...] = low
    copies[7].wait()
    ff = w_ref.shape[1]
    tile = halves_of(ff)
    for j in range(0, ff, tile):
        split_store(toks_ref[...], w_ref, kept_ref, sent_ref, slice(j, j + tile))


def low_part(blocks, shift, count, task, request, tokens, emb, gen_in, a, w, x):
    hidden, slab, rank = a.shape
    groups, rows = count.shape[1], request.shape[1]
    width, ff = w.shape
    a = a.transpose(0, 2, 1).reshape(hidden * rank, slab)
    vmem = pl.BlockSpec(memory_space=pltpu.VMEM)
    hbm = pl.BlockSpec(memory_space=pltpu.HBM)
    moved = (count, task, request, tokens, emb, gen_in, a, w)
    extra = () if x is None else (x,)
    return pl.pallas_call(
        functools.partial(low_kernel, blocks, slab, shift),
        in_specs=[hbm] * len(moved) + [vmem] * len(extra),
        out_specs=[vmem] * 6,
        out_shape=(
            jax.ShapeDtypeStruct((rank, rows), F32),
            jax.ShapeDtypeStruct((groups, hidden), BF16),
            jax.ShapeDtypeStruct((groups, rows // 2), BF16),
            jax.ShapeDtypeStruct((rows, width), BF16),
            jax.ShapeDtypeStruct((rows // 2, ff), F32),
            jax.ShapeDtypeStruct((rows // 2, ff), BF16),
        ),
        scratch_shapes=[pltpu.VMEM(m.shape, m.dtype) for m in moved]
        + [pltpu.VMEM((hidden, rows), F32), pltpu.SemaphoreType.DMA((len(moved),))],
        compiler_params=pltpu.CompilerParams(vmem_limit_bytes=36 << 20),
        name="low_part",
    )(*[stay(m) for m in moved], *extra)


def split_kernel(x_ref, w_ref, kept_ref, sent_ref):
    split_store(x_ref[...], w_ref, kept_ref, sent_ref, slice(None))


def split_matmul(x, w):
    rows, width = x.shape
    ff = w.shape[1]
    tile = halves_of(ff)
    return pl.pallas_call(
        split_kernel,
        grid=(ff // tile,),
        in_specs=[
            pl.BlockSpec((rows, width), lambda i: (0, 0)),
            pl.BlockSpec((width, tile), lambda i: (0, i)),
        ],
        out_specs=[
            pl.BlockSpec((rows // 2, tile), lambda i: (0, i)),
            pl.BlockSpec((rows // 2, tile), lambda i: (0, i)),
        ],
        out_shape=(
            pltpu.VMEM((rows // 2, ff), F32),
            jax.ShapeDtypeStruct((rows // 2, ff), BF16),
        ),
        compiler_params=pltpu.CompilerParams(vmem_limit_bytes=16 << 20),
    )(x, w)


def factor_kernel(hyper_ref, gen_ref, out_ref, wide_ref):
    hidden, ranks, tile = gen_ref.shape
    groups = hyper_ref.shape[0]

    @pl.when(pl.program_id(0) == 0)
    def _():
        part = 128
        spread = part * ranks
        lane = lax.broadcasted_iota(jnp.int32, (part, spread), 1)
        first = lax.broadcasted_iota(jnp.int32, (part, spread), 0) * ranks
        repeat = ((lane >= first) & (lane < first + ranks)).astype(F32).astype(BF16)
        which = lax.rem(lax.broadcasted_iota(jnp.int32, (groups, spread), 1), ranks)
        for k in range(hidden // part):
            wide = jnp.dot(
                hyper_ref[:, k * part : (k + 1) * part], repeat, preferred_element_type=F32
            )
            for r in range(ranks):
                wide_ref[r * groups : (r + 1) * groups, k * spread : (k + 1) * spread] = jnp.where(
                    which == r, wide, 0.0
                ).astype(BF16)

    out_ref[...] = jnp.dot(
        wide_ref[...], gen_ref[...].reshape(hidden * ranks, tile), preferred_element_type=F32
    ).astype(BF16)


def factors(hyper, gen_b):
    hidden, ranks, ff = gen_b.shape
    groups = hyper.shape[0]
    tile = halves_of(ff)
    return pl.pallas_call(
        factor_kernel,
        grid=(ff // tile,),
        in_specs=[
            pl.BlockSpec((groups, hidden), lambda i: (0, 0)),
            pl.BlockSpec((hidden, ranks, tile), lambda i: (0, 0, i)),
        ],
        out_specs=pl.BlockSpec((ranks * groups, tile), lambda i: (0, i)),
        out_shape=jax.ShapeDtypeStruct((ranks * groups, ff), BF16),
        scratch_shapes=[pltpu.VMEM((ranks * groups, hidden * ranks), BF16)],
        compiler_params=pltpu.CompilerParams(vmem_limit_bytes=24 << 20),
        name="factors",
    )(hyper, gen_b)


def delta_kernel(pieces, low_ref, member_ref, mine_ref, peer_ref, kept_ref, got_ref, sum_ref, *sent):
    groups = member_ref.shape[0]
    ranks = mine_ref.shape[0] // groups
    member = member_ref[...].astype(F32)
    total = kept_ref[...] + got_ref[...].astype(F32)
    for which, factor in ((0, mine_ref), (1, peer_ref)):
        first = (lax.axis_index(ROW) ^ which) * ranks
        spread = jnp.concatenate(
            [
                (member * low_ref[pl.ds(first + r, 1), :].astype(BF16).astype(F32)).astype(BF16)
                for r in range(ranks)
            ],
            axis=0,
        )
        total += lax.dot_general(
            spread, factor[...], (((0,), (0,)), ((), ())), preferred_element_type=F32
        )
    sum_ref[...] = total
    total = total.astype(BF16)
    for (start, size), ref in zip(pieces, sent):
        ref[...] = total[start : start + size]


def add_adapter(pieces, low, member, mine, peer, kept, got):
    rows, ff = kept.shape
    tile = halves_of(ff)
    whole = lambda x: pl.BlockSpec(x.shape, lambda i: (0, 0))
    cut = lambda n: pl.BlockSpec((n, tile), lambda i: (0, i))
    return pl.pallas_call(
        functools.partial(delta_kernel, pieces),
        grid=(ff // tile,),
        in_specs=[whole(low), whole(member)] + [cut(x.shape[0]) for x in (mine, peer, kept, got)],
        out_specs=[cut(rows)] + [cut(size) for _, size in pieces],
        out_shape=[pltpu.VMEM((rows, ff), F32)]
        + [jax.ShapeDtypeStruct((size, ff), BF16) for _, size in pieces],
        compiler_params=pltpu.CompilerParams(vmem_limit_bytes=16 << 20),
        name="adapter",
    )(low, member, mine, peer, kept, got)


def gate_kernel(kept_ref, core_ref, rest_ref, later_ref, out_ref):
    gate = kept_ref[...] + core_ref[...].astype(F32) + rest_ref[...].astype(F32)
    out_ref[...] = gate * (1.0 / (1.0 + jnp.exp(-gate)))


def activate(kept, core_got, rest, later):
    return in_vmem(gate_kernel, pltpu.VMEM(kept.shape, F32), kept, core_got, rest, later)


def in_vmem(kernel, out, *args, scratch=()):
    vmem = pl.BlockSpec(memory_space=pltpu.VMEM)
    return pl.pallas_call(
        kernel,
        in_specs=[vmem] * len(args),
        out_specs=jax.tree.map(lambda _: vmem, out),
        out_shape=out,
        scratch_shapes=scratch,
        compiler_params=pltpu.CompilerParams(vmem_limit_bytes=8 << 20),
    )(*args)


def split_rows(hid_ref, w_ref):
    acc = jnp.dot(hid_ref[...], w_ref[...], preferred_element_type=F32)
    col = lax.axis_size(COL)
    acc = acc.reshape(col // 2, 2, acc.shape[0] // col, acc.shape[1])
    low_bit = (lax.axis_index(COL) & 1) == 0
    keep = jnp.where(low_bit, acc[:, 0], acc[:, 1])
    give = jnp.where(low_bit, acc[:, 1], acc[:, 0])
    return keep, give.astype(BF16)


def down_kernel(hid_ref, w_ref, keep_ref, give_ref):
    keep_ref[...], give_ref[...] = split_rows(hid_ref, w_ref)


def cross_kernel(hid_ref, w_ref, own_keep_ref, own_give_ref, keep_ref, give_ref):
    keep_ref[0], give_ref[0] = own_keep_ref[...], own_give_ref[...]
    keep_ref[1], give_ref[1] = split_rows(hid_ref, w_ref)


def down(hid, w):
    col = lax.axis_size(COL)
    shape = (col // 2, hid.shape[0] // col, w.shape[1])
    out = (jax.ShapeDtypeStruct(shape, F32), jax.ShapeDtypeStruct(shape, BF16))
    return in_vmem(down_kernel, out, hid, w)


def cross(other, w, own):
    out = tuple(jax.ShapeDtypeStruct((2,) + x.shape, x.dtype) for x in own)
    return in_vmem(cross_kernel, out, other, w, *own)


def turned_split(hid_ref, w_ref, scratch):
    acc = jnp.dot(hid_ref[...], w_ref[...], preferred_element_type=F32)
    col = lax.axis_size(COL)
    scratch[...] = acc.reshape(col // 2, 2, acc.shape[0] // col, acc.shape[1])
    here = lax.axis_index(COL) >> 1
    return [scratch[pl.ds(here ^ q, 1)][0] for q in range(4)]


def turned_down_kernel(hid_ref, w_ref, *refs):
    for part, ref in zip(turned_split(hid_ref, w_ref, refs[4]), refs):
        ref[...] = part.astype(ref.dtype)


def turned_cross_kernel(hid_ref, w_ref, *refs):
    for part, own, ref in zip(turned_split(hid_ref, w_ref, refs[8]), refs[:4], refs[4:]):
        ref[0] = own[...]
        ref[1] = part.astype(ref.dtype)


def turned_down(hid, w, own):
    col = lax.axis_size(COL)
    shape = (2, hid.shape[0] // col, w.shape[1])
    scratch = [pltpu.VMEM((col // 2,) + shape, F32)]
    lead = () if own is None else (2,)
    out = [jax.ShapeDtypeStruct(lead + shape, F32 if q == 0 else BF16) for q in range(4)]
    kernel, own = (turned_down_kernel, ()) if own is None else (turned_cross_kernel, own)
    return in_vmem(kernel, out, hid, w, *own, scratch=scratch)


def turned_fold_kernel(total_ref, *refs):
    side = lax.axis_index(COL) & 1
    for ref, which in ((refs[3], side), (refs[4], 1 - side)):
        at = pl.ds(which, 1)
        value = total_ref[:, at]
        for got in refs[:3]:
            value += got[:, at].astype(F32)
        ref[...] = value.astype(ref.dtype)


def turned_fold(total, gots):
    shape = total.shape[:1] + (1,) + total.shape[2:]
    out = (jax.ShapeDtypeStruct(shape, F32), jax.ShapeDtypeStruct(shape, BF16))
    return in_vmem(turned_fold_kernel, out, total, *gots)


def fold_kernel(bit, keep_ref, got_ref, new_ref, give_ref):
    parts = keep_ref.shape[1]
    side = (lax.axis_index(COL) >> bit) & 1
    for j in range(parts // 2):
        for ref, which in ((new_ref, side), (give_ref, 1 - side)):
            at = pl.ds(2 * j + which, 1)
            ref[:, j : j + 1] = (keep_ref[:, at] + got_ref[:, at].astype(F32)).astype(ref.dtype)


def fold(bit, keep, got):
    shape = keep.shape[:1] + (keep.shape[1] // 2,) + keep.shape[2:]
    out = (jax.ShapeDtypeStruct(shape, F32), jax.ShapeDtypeStruct(shape, BF16))
    return in_vmem(functools.partial(fold_kernel, bit), out, keep, got)


def last_kernel(bit, count, *refs):
    here = lax.axis_index(COL) >> bit
    start = 0
    for k in range(count):
        keep_ref, got_ref = refs[2 * k : 2 * k + 2]
        rows = slice(start, start + keep_ref.shape[2])
        for q, ref in enumerate(refs[2 * count :]):
            at = pl.ds(here ^ q, 1)
            ref[:, :, rows] = (keep_ref[:, at] + got_ref[:, at].astype(F32)).astype(ref.dtype)
        start = rows.stop


def last_split(bit, parts):
    keep = parts[0][0]
    shape = keep.shape[:1] + (1, sum(k.shape[2] for k, _ in parts)) + keep.shape[3:]
    out = [jax.ShapeDtypeStruct(shape, F32)] + [jax.ShapeDtypeStruct(shape, BF16)] * 3
    kernel = functools.partial(last_kernel, bit, len(parts))
    return in_vmem(kernel, out, *[x for part in parts for x in part])


def join_kernel(counts, *refs):
    out_ref = refs[-1]
    requests, draft, width = out_ref.shape
    core = lax.axis_index(ROW) & 1
    start = 0
    for count in counts:
        (total, *got), refs = refs[:count], refs[count:]
        for side in range(2):
            if got:
                value = total[side, 0]
                for g in got:
                    value += g[side, 0].astype(F32)
                size = value.shape[0] // draft
                value = value.astype(BF16).reshape(size, draft, width)
            else:
                value = total[side]
                size = value.shape[0]
            at = start + (requests // 2) * (core if side == 0 else 1 - core)
            out_ref[pl.ds(at, size)] = value
        start += size


def settle_kernel(*refs):
    total_ref, *got_refs, out_ref = refs
    draft = out_ref.shape[2]
    value = total_ref[:, 0]
    for got in got_refs:
        value += got[:, 0].astype(F32)
    size, width = value.shape[1:]
    for side in range(2):
        out_ref[side] = value[side].astype(BF16).reshape(size // draft, draft, width)


def settle(part, draft):
    _, _, size, width = part[0].shape
    out = jax.ShapeDtypeStruct((2, size // draft, draft, width), BF16)
    return [in_vmem(settle_kernel, out, *part)]


def join(parts, out):
    kernel = functools.partial(join_kernel, tuple(len(p) for p in parts))
    return in_vmem(kernel, out, *[x for p in parts for x in p])


def hidden_kernel(start, act_ref, half_ref, up_ref, out_ref):
    at = slice(start, start + out_ref.shape[0])
    out_ref[...] = (act_ref[at] * (half_ref[at] + up_ref[...].astype(F32))).astype(BF16)


def hidden_units(piece, act, half, up_got):
    start, size = piece
    out = jax.ShapeDtypeStruct((size, act.shape[1]), BF16)
    return in_vmem(functools.partial(hidden_kernel, start), out, act, half, up_got)


def shards(tokens, task_emb, gen_in, gen_a, gen_b, w_gate, w_up, w_down, group_count, group_task):
    batch, draft, _ = tokens.shape
    rows = batch * draft
    rn, cn = lax.axis_size(ROW), lax.axis_size(COL)
    ri, ci = lax.axis_index(ROW), lax.axis_index(COL)
    core = ri & 1
    rmasks, cmasks = masks_of(rn), masks_of(cn)
    slab = gen_a.shape[1]

    per_dest = rows // cn
    chunks, joint, turned = plan(per_dest)
    turned = turned and len(cmasks) == 3
    sizes = [per_dest * part // sum(chunks) for part in chunks]
    blocks, pieces, target, source = [], [], 0, 0
    for size in sizes:
        pieces.append((target, cn * size // 2))
        for d in range(cn):
            blocks.append(((d * per_dest + source) // draft, target, size // 2))
            target += size // 2
        source += size // 2
    shift = per_dest // 2 // draft

    request = np.concatenate([begin + np.arange(size) // draft for begin, _, size in blocks])
    request = np.concatenate([request, request])[None, :].astype(np.int32)
    x = None
    if slab % 128:
        x = lax.dynamic_slice_in_dim(tokens, ci * slab, slab, 2)
        x = jnp.concatenate(
            [
                lax.dynamic_slice_in_dim(x, begin + shift * side, size // draft).reshape(size, slab)
                for side in (core, 1 - core)
                for begin, _, size in blocks
            ]
        )
    low, hyper, own_member, toks, gate_kept, gate_sent = low_part(
        tuple(blocks),
        shift,
        group_count[None, :],
        group_task[None, :],
        jnp.asarray(request),
        tokens,
        task_emb,
        gen_in,
        gen_a,
        w_gate,
        x,
    )
    gate_got = swap(gate_sent, ROW, 1)
    for m in rmasks[1:]:
        low = low + swap(low, ROW, m)
    gate_sum = (gate_kept + gate_got.astype(F32)).astype(BF16)

    def others(sent):
        total = None
        for s, m in enumerate(rmasks[1:]):
            got = swap(sent, ROW, m)
            if s + 2 == len(rmasks) and total is None:
                return got
            total = got.astype(F32) if total is None else total + got.astype(F32)
            sent = (sent.astype(F32) + got.astype(F32)).astype(BF16)
        return total

    gate_rest = others(gate_sum)

    up_kept, up_sent = split_matmul(toks, w_up)
    up_got = swap(up_sent, ROW, 1)
    b_mine = factors(hyper, gen_b)
    b_peer = swap(b_mine, ROW, 1)
    for m in cmasks[:-2]:
        low = low + swap(low, COL, m)
    gots = [swap(low, COL, q * cmasks[-2]) for q in (1, 2, 3)]
    low = low + gots[0] + gots[1] + gots[2]
    low = low[:, : rows // 2] + swap(low[:, rows // 2 :], ROW, 1)

    up_half, *up_sums = add_adapter(
        tuple(pieces), low, own_member, b_mine, b_peer, up_kept, up_got
    )

    act = activate(gate_kept, gate_got, gate_rest, w_down)
    outs = []
    for k, piece in enumerate(pieces):
        up_rest = others(up_sums[k])
        hid = hidden_units(piece, act, up_half, up_rest)
        other = swap(hid, ROW, 1)
        if k == 0 and turned:
            own = turned_down(hid, w_down, None)
            total, *gives = turned_down(other, w_down, own)
            gots = [swap(give, COL, (q + 1) << 1) for q, give in enumerate(gives)]
            keep, give = turned_fold(total, gots)
            first = [keep, swap(give, COL, 1)]
            outs.append(None)
            continue
        keep, give = cross(other, w_down, down(hid, w_down))
        for s, m in enumerate(cmasks[:-2]):
            got = swap(give, COL, m)
            if s + 3 < len(cmasks):
                keep, give = fold(s + 1, keep, got)
        outs.append((keep, got))
    low_bit = len(cmasks) - 2
    parts = [first] if turned else []
    for members in joint:
        total, *gives = last_split(low_bit, [outs[k] for k in members])
        gots = [swap(give, COL, (q + 1) << low_bit) for q, give in enumerate(gives)]
        parts.append([total] + gots)
    parts = [settle(p, draft) for p in parts[:-1]] + parts[-1:]
    return join(parts, jax.ShapeDtypeStruct((batch // cn, draft, w_down.shape[1]), BF16))


def solution(mesh):
    in_specs = (
        P(None, None, ROW),
        P(),
        P(),
        P(None, (ROW, COL), None),
        P(None, ROW, COL),
        P(ROW, COL),
        P(ROW, COL),
        P(COL, ROW),
        P(),
        P(),
    )
    out_specs = P(COL, None, ROW)

    return jax.shard_map(shards, mesh=mesh, in_specs=in_specs, out_specs=out_specs, check_vma=False)
```
